256 devices in a mesh: groups: 2 (over y), shard: 128 (over z, x, core).
Axes of the slice: x: 4, y: 2, z: 16, core: 2. Of those that a mesh axis runs over, the one named last changes fastest.
The devices are a block of a 4x16x16 slice.
Arguments:
- query_tokens: bfloat16 [8192, 32, 128], P(('groups', 'shard')), parts along dimension 0, may hold values from -0.1875 to 0.1875
- candidates: int32 [8192, 24], P(('groups', 'shard')), parts along dimension 0, may hold values from 0 to 4095, as said below
- cand_count: int32 [8192], P(('groups', 'shard')), parts along dimension 0, may hold values from 3 to 24, as said below
- placement_map: int32 [8192], P('groups'), parts along dimension 0, may hold values from 0 to 4095, as said below
- passage_base: bfloat16 [8192, 128, 128], P(('groups', 'shard')), parts along dimension 0, may hold values from -6 to 6
- residual_codes: int32 [8192, 128, 128], P(('groups', 'shard')), parts along dimension 0, may hold values from 0 to 3
- passage_lengths: int32 [8192], P(('groups', 'shard')), parts along dimension 0, may hold values from 32 to 128
- bucket_weights: float32 [8], P('groups'), parts along dimension 0, may hold values from -3 to 3
Outputs:
- scores: float32 [8192, 24], P(('groups', 'shard')), parts along dimension 0
The draws below stay inside these ranges and needn't reach their ends.
There are 2 independent parts, one for each index of `groups`. The reference program is written for one: setup_inputs(seed, part) draws one part's arguments, and reference() takes and returns one part's arrays. A program takes and returns all parts, laid end to end along the dimension named above; each array names one. Nothing has to cross between parts.
Inputs may be any that keep to these rules, and one draw needn't show every extreme that they name: In row q the first cand_count[q] entries are distinct passage ids; the devices that store them (device placement_map[id] // 32 of the shard axis) are at most 3, and one device stores at most 8 of them. Of the 32 queries of one device, one storing device (the same for all devices) holds candidates of exactly 3, and every other storing device holds candidates of at most 1. Entries at or beyond cand_count[q] are arbitrary ids. `cand_count`: entries of candidates at or beyond this count are not scored. A permutation: passage id p is row placement_map[p] of the passage store.
All inputs are finite; a program needn't handle non-finite values.
Results may differ from the reference program's by a relative error of at most 0.0003.
Values may be sent and summed in bfloat16 or wider, within the bound.
No kernel may reach another device: no remote copies, remote signals or barrier semaphores. Data moves between devices by JAX's collectives and lax.ppermute only.
A program may use at most 64 MiB of HBM per device.

```python
import jax
import jax.numpy as jnp
from jax import lax

DIM = 128
QLEN = 32
PLEN = 128
OWNERS_Q = 3
CPQ = 8
Q_DEV = 32
P_DEV = 32
NQ = 4096
P_TOTAL = 4096
CMAX = 24
HOTQ = 3
N_SHARD = 128


def layout(key):
    device_count = N_SHARD
    folded = jax.random.fold_in(key, 911)
    streams = jax.random.split(folded, 8)
    placed = jax.random.permutation(streams[0], P_TOTAL).astype(jnp.int32)
    inverse = jnp.argsort(placed).astype(jnp.int32)
    hottest = jax.random.randint(streams[1], (), 0, device_count, dtype=jnp.int32)
    others = jax.random.permutation(streams[2], device_count - 1).astype(jnp.int32)
    others = others + (others >= hottest).astype(jnp.int32)
    offset = jax.random.randint(streams[3], (device_count, 1, 1), 0, Q_DEV, dtype=jnp.int32)
    query_idx = jnp.arange(Q_DEV, dtype=jnp.int32)[None, :, None]
    owner_idx = jnp.arange(OWNERS_Q, dtype=jnp.int32)[None, None, :]
    turned = (query_idx - offset) % Q_DEV
    is_hot = (owner_idx == 0) & (turned < HOTQ)
    prior_offset = jnp.minimum(turned + (owner_idx > 0).astype(jnp.int32), HOTQ)
    position = turned * OWNERS_Q + owner_idx - prior_offset
    holders = jnp.where(is_hot, hottest, others[position % (device_count - 1)])
    filled = is_hot | (turned == 0)
    shape3 = (device_count, Q_DEV, OWNERS_Q)
    counts = jnp.where(filled, CPQ, jax.random.randint(streams[4], shape3, 1, CPQ + 1, dtype=jnp.int32))
    ranking = jax.random.randint(streams[5], shape3 + (P_DEV,), 0, 4096, dtype=jnp.int32) * P_DEV + jnp.arange(P_DEV, dtype=jnp.int32)
    picked_rows = jnp.argsort(ranking, axis=-1)[..., :CPQ].astype(jnp.int32)
    chosen = inverse[holders[..., None] * P_DEV + picked_rows]
    usable = jnp.arange(CPQ, dtype=jnp.int32) < counts[..., None]
    filler = jax.random.randint(streams[6], shape3 + (CPQ,), 0, P_TOTAL, dtype=jnp.int32)
    chosen = jnp.where(usable, chosen, filler).reshape(device_count, Q_DEV, CMAX)
    usable = usable.reshape(device_count, Q_DEV, CMAX)
    mixing = jax.random.randint(streams[7], (device_count, Q_DEV, CMAX), 0, 4096, dtype=jnp.int32) * CMAX + jnp.arange(CMAX, dtype=jnp.int32)
    sort_key = jnp.where(usable, 0, 4096 * CMAX) + mixing
    picked = jnp.argsort(sort_key, axis=-1)
    chosen = jnp.take_along_axis(chosen, picked, axis=-1)
    totals = jnp.sum(counts, axis=-1).astype(jnp.int32)
    return (placed, chosen.reshape(NQ, CMAX), totals.reshape(NQ))


def draw_candidates(key, part):
    return layout(key)[1]


def draw_cand_count(key, part):
    return layout(key)[2]


def draw_placement_map(key, part):
    return layout(key)[0]


def touch_ends(array, key, smallest, largest):
    spot = [jax.random.randint(jax.random.fold_in(key, axis), (), 0, length) for axis, length in enumerate(array.shape)]
    longest = array.shape.index(max(array.shape))
    neighbour = spot[:longest] + [(spot[longest] + 1) % array.shape[longest]] + spot[longest + 1:]
    return array.at[tuple(spot)].set(smallest).at[tuple(neighbour)].set(largest)


def level_of(stream_key, dims, shards, least, largest):
    loudness, own = 1.0, jax.random.fold_in(stream_key, 6)
    for dim, shards_of in shards:
        heights = jnp.exp(jax.random.uniform(jax.random.fold_in(own, dim), (shards_of,), jnp.float32, least / len(shards), largest / len(shards)))
        loudness = loudness * jnp.repeat(heights, dims[dim] // shards_of).reshape([-1 if axis == dim else 1 for axis in range(len(dims))])
    return loudness


def bell_draw(stream_key, dims, scale, bound, shards=(), held_as=jnp.bfloat16):
    factor_of = level_of(stream_key, dims, shards, -0.22, 0.18) if shards else 1.0
    entries = jax.random.normal(stream_key, dims, jnp.float32) * scale * factor_of
    return jnp.minimum(jnp.maximum(entries, -bound), bound).astype(held_as)


def setup_inputs(seed: int = 0, part: int = 0) -> dict:
    splits = jax.random.split(jax.random.key(seed), 9)
    part_keys = jax.random.split(jax.random.fold_in(splits[8], part), 9)
    return {
        "query_tokens": bell_draw(part_keys[0], (NQ, QLEN, DIM), (1.0 / QLEN), 0.1875, ((0, 128),)),
        "candidates": draw_candidates(jax.random.fold_in(jax.random.fold_in(splits[8], part), 71), part),
        "cand_count": draw_cand_count(jax.random.fold_in(jax.random.fold_in(splits[8], part), 71), part),
        "placement_map": draw_placement_map(jax.random.fold_in(jax.random.fold_in(splits[8], part), 71), part),
        "passage_base": bell_draw(part_keys[4], (P_TOTAL, PLEN, DIM), 1.0, 6.0, ((0, 128),)),
        "residual_codes": touch_ends(jax.random.randint(part_keys[5], (P_TOTAL, PLEN, DIM), 0, 4), jax.random.fold_in(part_keys[5], 1), 0, 3).astype(jnp.int32),
        "passage_lengths": touch_ends(jax.random.randint(part_keys[6], (P_TOTAL,), PLEN // 4, PLEN + 1), jax.random.fold_in(part_keys[6], 1), PLEN // 4, PLEN).astype(jnp.int32),
        "bucket_weights": bell_draw(part_keys[7], (4,), 0.5, 3.0, (), jnp.float32),
    }


epsilon = 1e-06
negative = -1e+30

def decode(bases, code_ids, levels):
    residual = jnp.zeros(bases.shape, jnp.float32)
    for bucket in range(4):
        residual = residual + jnp.where(code_ids == bucket, levels[bucket], 0.0)
    summed = bases.astype(jnp.float32) + residual
    inverse_norm = lax.rsqrt(lax.optimization_barrier(jnp.sum(summed * summed, axis=-1, keepdims=True)) + epsilon)
    return (summed * inverse_norm).astype(jnp.bfloat16)

def reference(query_tokens, candidates, cand_count, placement_map, passage_base, residual_codes, passage_lengths, bucket_weights):

    def decode_block(bundle):
        return decode(bundle[0], bundle[1], bucket_weights)
    decoded = lax.map(decode_block, (passage_base.reshape(N_SHARD, P_DEV, PLEN, DIM), residual_codes.reshape(N_SHARD, P_DEV, PLEN, DIM)))
    decoded = decoded.reshape(P_TOTAL, PLEN, DIM)

    def score_block(bundle):
        query_rows, listed, counted = bundle
        stored = placement_map[listed]
        token_rows = decoded[stored].astype(jnp.float32)
        lengths = passage_lengths[stored]
        similarity_scores = jnp.einsum('tug,terg->tuer', query_rows.astype(jnp.float32), token_rows)
        inside = jnp.arange(PLEN, dtype=jnp.int32)[None, None, None, :] < lengths[:, None, :, None]
        maxima = lax.optimization_barrier(jnp.max(jnp.where(inside, similarity_scores, negative), axis=3))
        summed = lax.optimization_barrier(jnp.sum(maxima, axis=1))
        usable = jnp.arange(CMAX, dtype=jnp.int32)[None, :] < counted[:, None]
        return jnp.where(usable, summed, 0.0)
    scored = lax.map(score_block, (query_tokens.reshape(N_SHARD, Q_DEV, QLEN, DIM), candidates.reshape(N_SHARD, Q_DEV, CMAX), cand_count.reshape(N_SHARD, Q_DEV)))
    return scored.reshape(NQ, CMAX)
```

```python
import functools

import jax
import jax.numpy as jnp
from jax import lax
from jax.experimental import pallas as pl
from jax.experimental.pallas import tpu as pltpu
from jax.sharding import PartitionSpec as P

EPSILON = 1e-06
PLANE = 8
F32 = jnp.float32
BF16 = jnp.bfloat16


def vmem(*_):
    return pl.BlockSpec(memory_space=pltpu.VMEM)


def smem(*_):
    return pl.BlockSpec(memory_space=pltpu.SMEM)


def cost(flops, moved):
    return pl.CostEstimate(flops=flops, transcendentals=0, bytes_accessed=moved)


def columns(parts, width):
    lane = lax.broadcasted_iota(jnp.int32, (parts[0].shape[0], width), 1)
    out = jnp.zeros((parts[0].shape[0], width), F32)
    for index, part in enumerate(parts):
        out = jnp.where(lane == index, part, out)
    return out


def prepare_kernel(
    store_rows, device_count,
    cand_ref, count_ref, map_ref, query_ref,
    out_ref, holder_ref, row_ref, busiest_ref,
    pick_vmem, pick_smem, sem,
):
    queries, slots = cand_ref.shape
    table_rows, lanes = map_ref.shape
    table = map_ref[...]
    holder_table = table // store_rows
    row_table = table - holder_table * store_rows
    both = jnp.concatenate([holder_table, row_table], axis=1).astype(F32).astype(BF16)
    ids = cand_ref[...]
    high = ids // lanes
    low = ids - high * lanes
    table_iota = lax.broadcasted_iota(jnp.int32, (queries, table_rows), 1)
    lane_iota = lax.broadcasted_iota(jnp.int32, (queries, lanes), 1)
    device_iota = lax.broadcasted_iota(jnp.int32, (queries, device_count), 1)
    marks = [
        jnp.where(table_iota == high[:, c : c + 1], 1.0, 0.0) for c in range(slots)
    ]
    rows = jnp.dot(
        jnp.concatenate(marks, axis=0).astype(BF16), both, preferred_element_type=F32
    )
    present = jnp.zeros((queries, device_count), F32)
    holders, local_rows = [], []
    for c in range(slots):
        block = rows[c * queries : (c + 1) * queries]
        here = lane_iota == low[:, c : c + 1]
        holder = jnp.sum(jnp.where(here, block[:, :lanes], 0.0), axis=1, keepdims=True)
        row = jnp.sum(jnp.where(here, block[:, lanes:], 0.0), axis=1, keepdims=True)
        holder = jnp.where(count_ref[...] > c, holder, -1.0)
        present = jnp.where(device_iota == holder.astype(jnp.int32), 1.0, present)
        holders.append(holder)
        local_rows.append(row)
    holder_ref[...] = columns(holders, slots)
    row_ref[...] = columns(local_rows, slots)
    query_iota = lax.broadcasted_iota(jnp.int32, (queries, device_count), 0).astype(F32)
    pick = jnp.max(present * query_iota, axis=0, keepdims=True)
    pick_vmem[...] = jnp.broadcast_to(pick.astype(jnp.int32), pick_vmem.shape)
    copy = pltpu.make_async_copy(pick_vmem, pick_smem, sem)
    copy.start()
    shared = jnp.sum(present, axis=0, keepdims=True)
    device = lax.broadcasted_iota(jnp.int32, (1, device_count), 1).astype(F32)
    busiest_ref[0] = jnp.max(jnp.where(shared > 1.5, device, 0.0)).astype(jnp.int32)
    copy.wait()

    def pack(step, carry):
        for inner in range(8):
            device = step * 8 + inner
            out_ref[device] = query_ref[pick_smem[0, device]]
        return carry

    lax.fori_loop(0, device_count // 8, pack, 0)


def prepare(candidates, cand_count, placement_map, query_tokens, store_rows, device_count):
    queries, slots = candidates.shape
    _, tokens, dim = query_tokens.shape
    return pl.pallas_call(
        functools.partial(prepare_kernel, store_rows, device_count),
        name="prepare",
        out_shape=(
            jax.ShapeDtypeStruct((device_count, tokens, dim), BF16),
            jax.ShapeDtypeStruct((queries, slots), F32),
            jax.ShapeDtypeStruct((queries, slots), F32),
            jax.ShapeDtypeStruct((1,), jnp.int32),
        ),
        in_specs=[vmem(), vmem(), vmem(), vmem()],
        out_specs=(vmem(), vmem(), vmem(), smem()),
        scratch_shapes=[
            pltpu.VMEM((8, device_count), jnp.int32),
            pltpu.SMEM((8, device_count), jnp.int32),
            pltpu.SemaphoreType.DMA(()),
        ],
    )(
        candidates,
        cand_count.reshape(queries, 1),
        placement_map.reshape(-1, 128),
        query_tokens,
    )


def decode_kernel(length_ref, level_ref, base_ref, code_ref, out_ref):
    step = pl.program_id(0)
    block, length, dim = base_ref.shape
    token = lax.broadcasted_iota(jnp.int32, (length, dim), 0)
    for index in range(block):
        code = code_ref[index]
        residual = jnp.where(
            code < 2,
            jnp.where(code == 0, level_ref[0], level_ref[1]),
            jnp.where(code == 2, level_ref[2], level_ref[3]),
        )
        summed = base_ref[index].astype(F32) + residual
        inverse = lax.rsqrt(jnp.sum(summed * summed, axis=1, keepdims=True) + EPSILON)
        tokens = summed * inverse
        tokens = jnp.where(token < length_ref[step * block + index], tokens, tokens[0:1])
        out_ref[index] = tokens.astype(BF16)


def decode(passage_base, residual_codes, passage_lengths, bucket_weights):
    rows, length, dim = passage_base.shape
    block = 8
    spec = pl.BlockSpec((block, length, dim), lambda i: (i, 0, 0))
    return pl.pallas_call(
        decode_kernel,
        name="decode",
        grid=(rows // block,),
        out_shape=jax.ShapeDtypeStruct(passage_base.shape, BF16),
        in_specs=[smem(), smem(), spec, spec],
        out_specs=spec,
        cost_estimate=cost(rows * length * dim * 20, rows * length * dim * 8),
    )(passage_lengths, bucket_weights, passage_base, residual_codes)


def score_kernel(query_ref, store_ref, out_ref, best_ref):
    group, tokens, dim = query_ref.shape
    rows, length, _ = store_ref.shape
    wide = group * tokens
    query = query_ref[...].reshape(wide, dim)

    def one(row):
        similar = lax.dot_general(
            store_ref[row], query, (((1,), (1,)), ((), ())), preferred_element_type=F32
        )
        best_ref[row] = jnp.max(similar.reshape(length // 8, 8, wide), axis=0)

    def some(step, carry):
        for inner in range(4):
            one(step * 4 + inner)
        return carry

    lax.fori_loop(0, rows // 4, some, 0)
    best = jnp.max(best_ref[...], axis=1)
    member = lax.broadcasted_iota(jnp.int32, (group, wide), 1) // tokens
    mine = lax.broadcasted_iota(jnp.int32, (group, wide), 0)
    picks = jnp.where(member == mine, 1.0, 0.0)
    out_ref[...] = lax.dot_general(
        picks, best, (((1,), (1,)), ((), ())),
        preferred_element_type=F32, precision=lax.Precision.HIGHEST,
    )


def score(queries, store):
    count, tokens, dim = queries.shape
    rows, length, _ = store.shape
    group = 8
    return pl.pallas_call(
        score_kernel,
        name="score",
        grid=(count // group,),
        out_shape=jax.ShapeDtypeStruct((count, rows), F32),
        in_specs=[
            pl.BlockSpec((group, tokens, dim), lambda i: (i, 0, 0)),
            pl.BlockSpec((rows, length, dim), lambda i: (0, 0, 0)),
        ],
        out_specs=pl.BlockSpec((group, rows), lambda i: (i, 0)),
        scratch_shapes=[pltpu.VMEM((rows, 8, group * tokens), F32)],
        cost_estimate=cost(
            2 * count * tokens * rows * length * dim,
            2 * (count * tokens + rows * length) * dim,
        ),
    )(queries, store)


def finish_kernel(busiest_ref, holder_ref, row_ref, back_ref, hot_ref, out_ref):
    queries, slots = holder_ref.shape
    device_count, rows = back_ref.shape
    back = back_ref[...]
    first = back.astype(BF16)
    rest = back - first.astype(F32)
    second = rest.astype(BF16)
    third = (rest - second.astype(F32)).astype(BF16)
    device_iota = lax.broadcasted_iota(jnp.int32, (queries, device_count), 1)
    row_iota = lax.broadcasted_iota(jnp.int32, (queries, rows), 1)
    holder_all = holder_ref[...].astype(jnp.int32)
    row_all = row_ref[...].astype(jnp.int32)
    marks = [
        jnp.where(device_iota == holder_all[:, c : c + 1], 1.0, 0.0)
        for c in range(slots)
    ]
    mark = jnp.concatenate(marks, axis=0).astype(BF16)
    away = (
        jnp.dot(mark, first, preferred_element_type=F32)
        + jnp.dot(mark, second, preferred_element_type=F32)
    ) + jnp.dot(mark, third, preferred_element_type=F32)
    hot = hot_ref[...]
    picked = []
    for c in range(slots):
        holder = holder_all[:, c : c + 1]
        found = jnp.where(
            holder == busiest_ref[0], hot, away[c * queries : (c + 1) * queries]
        )
        value = jnp.sum(
            jnp.where(row_iota == row_all[:, c : c + 1], found, 0.0),
            axis=1, keepdims=True,
        )
        picked.append(jnp.where(holder >= 0, value, 0.0))
    out_ref[...] = columns(picked, slots)


def finish(busiest, holder, row, back, hot):
    return pl.pallas_call(
        finish_kernel,
        name="finish",
        out_shape=jax.ShapeDtypeStruct(holder.shape, F32),
        in_specs=[smem(), vmem(), vmem(), vmem(), vmem()],
        out_specs=vmem(),
    )(busiest, holder, row, back, hot)


def spread(store, busiest, device_count):
    planes = device_count // PLANE
    me = lax.axis_index("shard")
    plane, seat = me // PLANE, me % PLANE
    source_plane, source_seat = busiest // PLANE, busiest % PLANE
    rows, length, dim = store.shape
    part = rows // PLANE
    groups = [[p * PLANE + s for s in range(PLANE)] for p in range(planes)]
    parts = lax.all_to_all(
        store, "shard", 0, 0, tiled=True, axis_index_groups=groups
    ).reshape(PLANE, part * length, dim)
    piece = lax.dynamic_index_in_dim(parts, source_seat, 0, keepdims=False)

    def from_plane(start):
        def run(value):
            have, hop = [start], planes // 2
            while hop:
                pairs = [
                    (p * PLANE + s, ((p + hop) % planes) * PLANE + s)
                    for p in have for s in range(PLANE)
                ]
                moved = lax.ppermute(value, "shard", pairs)
                fresh = (plane - start) % (2 * hop) == hop
                value = jnp.where(fresh, moved, value)
                have = have + [(p + hop) % planes for p in have]
                hop //= 2
            return value

        return run

    piece = lax.switch(source_plane, [from_plane(p) for p in range(planes)], piece)
    pieces = [piece]
    for turn in range(1, PLANE):
        pieces.append(
            lax.ppermute(
                piece, "shard",
                [
                    (p * PLANE + s, p * PLANE + (s + turn) % PLANE)
                    for p in range(planes) for s in range(PLANE)
                ],
            )
        )
    turned = jnp.stack(pieces)
    order = (seat - jnp.arange(PLANE, dtype=jnp.int32)) % PLANE
    return turned[order].reshape(rows, length, dim)


def local(
    query_tokens, candidates, cand_count, placement_map,
    passage_base, residual_codes, passage_lengths, bucket_weights,
):
    device_count = lax.axis_size("shard")
    store_rows = passage_base.shape[0]
    outgoing, holder, row, busiest = prepare(
        candidates, cand_count, placement_map, query_tokens, store_rows, device_count
    )
    arrived = lax.all_to_all(outgoing, "shard", 0, 0, tiled=True)
    store = decode(passage_base, residual_codes, passage_lengths, bucket_weights)
    hot_store = spread(store, busiest[0], device_count)
    visited = score(arrived, store)
    back = lax.all_to_all(visited, "shard", 0, 0, tiled=True)
    hot = score(query_tokens, hot_store)
    return finish(busiest, holder, row, back, hot)


def solution(mesh):
    whole = P(("groups", "shard"))
    return jax.shard_map(
        local,
        mesh=mesh,
        in_specs=(whole, whole, whole, P("groups"), whole, whole, whole, P("groups")),
        out_specs=whole,
        check_vma=False,
    )
```

```python
import functools

import jax
import jax.numpy as jnp
from jax import lax
from jax.experimental import pallas as pl
from jax.experimental.pallas import tpu as pltpu
from jax.sharding import PartitionSpec as P

EPSILON = 1e-06
PLANE = 8
F32 = jnp.float32
BF16 = jnp.bfloat16


def vmem(*_):
    return pl.BlockSpec(memory_space=pltpu.VMEM)


def smem(*_):
    return pl.BlockSpec(memory_space=pltpu.SMEM)


def cost(flops, moved):
    return pl.CostEstimate(flops=flops, transcendentals=0, bytes_accessed=moved)


def columns(parts, width):
    lane = lax.broadcasted_iota(jnp.int32, (parts[0].shape[0], width), 1)
    out = jnp.zeros((parts[0].shape[0], width), F32)
    for index, part in enumerate(parts):
        out = jnp.where(lane == index, part, out)
    return out


def prepare_kernel(
    store_rows, device_count,
    cand_ref, count_ref, map_ref, query_ref,
    out_ref, holder_ref, row_ref, note_ref,
    pick_vmem, pick_smem, sem,
):
    queries, slots = cand_ref.shape
    table_rows, lanes = map_ref.shape
    table = map_ref[...]
    holder_table = table // store_rows
    row_table = table - holder_table * store_rows
    both = jnp.concatenate([holder_table, row_table], axis=1).astype(F32).astype(BF16)
    ids = cand_ref[...]
    high = ids // lanes
    low = ids - high * lanes
    table_iota = lax.broadcasted_iota(jnp.int32, (queries, table_rows), 1)
    lane_iota = lax.broadcasted_iota(jnp.int32, (queries, lanes), 1)
    device_iota = lax.broadcasted_iota(jnp.int32, (queries, device_count), 1)
    marks = [
        jnp.where(table_iota == high[:, c : c + 1], 1.0, 0.0) for c in range(slots)
    ]
    rows = jnp.dot(
        jnp.concatenate(marks, axis=0).astype(BF16), both, preferred_element_type=F32
    )
    present = jnp.zeros((queries, device_count), F32)
    holders, local_rows = [], []
    for c in range(slots):
        block = rows[c * queries : (c + 1) * queries]
        here = lane_iota == low[:, c : c + 1]
        holder = jnp.sum(jnp.where(here, block[:, :lanes], 0.0), axis=1, keepdims=True)
        row = jnp.sum(jnp.where(here, block[:, lanes:], 0.0), axis=1, keepdims=True)
        holder = jnp.where(count_ref[...] > c, holder, -1.0)
        present = jnp.where(device_iota == holder.astype(jnp.int32), 1.0, present)
        holders.append(holder)
        local_rows.append(row)
    holder_ref[...] = columns(holders, slots)
    row_ref[...] = columns(local_rows, slots)
    query_iota = lax.broadcasted_iota(jnp.int32, (queries, device_count), 0).astype(F32)
    pick = jnp.max(present * query_iota, axis=0, keepdims=True)
    pick_vmem[...] = jnp.broadcast_to(pick.astype(jnp.int32), pick_vmem.shape)
    copy = pltpu.make_async_copy(pick_vmem, pick_smem, sem)
    copy.start()
    shared = jnp.sum(present, axis=0, keepdims=True)
    device = lax.broadcasted_iota(jnp.int32, (1, device_count), 1).astype(F32)
    busiest = jnp.max(jnp.where(shared > 1.5, device, 0.0)).astype(jnp.int32)
    theirs = jnp.where(device_iota == busiest, present, 0.0)
    last = jnp.max(theirs * query_iota).astype(jnp.int32)
    total = jnp.sum(theirs * query_iota).astype(jnp.int32)
    first = (queries - 1) - jnp.max(theirs * ((queries - 1) - query_iota)).astype(jnp.int32)
    middle = jnp.clip(total - first - last, 0, queries - 1)
    note_ref[0] = busiest
    note_ref[1] = first
    note_ref[2] = middle
    tokens = query_ref.shape[1]
    extra = 2 * tokens // PLANE
    spare = []
    for seat in range(PLANE):
        query = first if seat < PLANE // 2 else middle
        start = (seat % (PLANE // 2)) * extra
        spare.append(query_ref[query, start : start + extra, :])
    copy.wait()

    def pack(step, carry):
        for seat in range(PLANE):
            device = step * PLANE + seat
            out_ref[device, 0:tokens, :] = query_ref[pick_smem[0, device]]
            out_ref[device, tokens : tokens + extra, :] = spare[seat]
        return carry

    lax.fori_loop(0, device_count // PLANE, pack, 0)


def prepare(candidates, cand_count, placement_map, query_tokens, store_rows, device_count):
    queries, slots = candidates.shape
    _, tokens, dim = query_tokens.shape
    return pl.pallas_call(
        functools.partial(prepare_kernel, store_rows, device_count),
        name="prepare",
        out_shape=(
            jax.ShapeDtypeStruct((device_count, tokens + 2 * tokens // PLANE, dim), BF16),
            jax.ShapeDtypeStruct((queries, slots), F32),
            jax.ShapeDtypeStruct((queries, slots), F32),
            jax.ShapeDtypeStruct((4,), jnp.int32),
        ),
        in_specs=[vmem(), vmem(), vmem(), vmem()],
        out_specs=(vmem(), vmem(), vmem(), smem()),
        scratch_shapes=[
            pltpu.VMEM((8, device_count), jnp.int32),
            pltpu.SMEM((8, device_count), jnp.int32),
            pltpu.SemaphoreType.DMA(()),
        ],
        cost_estimate=cost(10**9, 2 * 10**6),
    )(
        candidates,
        cand_count.reshape(queries, 1),
        placement_map.reshape(-1, 128),
        query_tokens,
    )


def decode_kernel(seat_ref, length_ref, level_ref, base_ref, code_ref, out_ref):
    part, length, dim = base_ref.shape
    block = lax.rem(seat_ref[0] + pl.program_id(0), PLANE)
    token = lax.broadcasted_iota(jnp.int32, (length, dim), 0)
    for index in range(part):
        code = code_ref[index]
        residual = jnp.where(
            code < 2,
            jnp.where(code == 0, level_ref[0], level_ref[1]),
            jnp.where(code == 2, level_ref[2], level_ref[3]),
        )
        summed = base_ref[index].astype(F32) + residual
        inverse = lax.rsqrt(jnp.sum(summed * summed, axis=1, keepdims=True) + EPSILON)
        tokens = summed * inverse
        tokens = jnp.where(token < length_ref[block * part + index], tokens, tokens[0:1])
        out_ref[0, index] = tokens.astype(BF16)


def decode(seat, passage_base, residual_codes, passage_lengths, bucket_weights):
    rows, length, dim = passage_base.shape
    part = rows // PLANE
    spec = pl.BlockSpec(
        (part, length, dim), lambda i, seat_ref: (lax.rem(seat_ref[0] + i, PLANE), 0, 0)
    )
    return pl.pallas_call(
        decode_kernel,
        name="decode",
        out_shape=jax.ShapeDtypeStruct((PLANE, part, length, dim), BF16),
        grid_spec=pltpu.PrefetchScalarGridSpec(
            num_scalar_prefetch=1,
            grid=(PLANE,),
            in_specs=[smem(), smem(), spec, spec],
            out_specs=pl.BlockSpec((1, part, length, dim), lambda i, _: (i, 0, 0, 0)),
        ),
        cost_estimate=cost(rows * length * dim * 20, rows * length * dim * 8),
    )(seat, passage_lengths, bucket_weights, passage_base, residual_codes)


def score_kernel(seat_ref, arrived_ref, store_ref, *refs):
    hot_refs, (out_ref, best_ref) = refs[:PLANE], refs[PLANE:]
    slots, height, dim = arrived_ref.shape
    _, part, length, _ = store_ref.shape
    rows = PLANE * part
    tokens = height * PLANE // (PLANE + 2)
    extra = height - tokens
    group = slots * extra // tokens
    wide = group * tokens
    seat = seat_ref[0]

    def against(query, block, turned, sign):
        for k in range(PLANE):
            home = lax.rem(seat + sign * k + PLANE, PLANE) * part
            for j in range(part):
                similar = lax.dot_general(
                    block(k, j), query, (((1,), (1,)), ((), ())),
                    preferred_element_type=F32,
                )
                best_ref[home + j] = jnp.max(similar.reshape(length // 8, 8, wide), axis=0)
        best = jnp.max(best_ref[...], axis=1)
        count = wide // turned
        member = lax.broadcasted_iota(jnp.int32, (count, wide), 1) // turned
        mine = lax.broadcasted_iota(jnp.int32, (count, wide), 0)
        picks = jnp.where(member == mine, 1.0, 0.0)
        return lax.dot_general(
            picks, best, (((1,), (1,)), ((), ())),
            preferred_element_type=F32, precision=lax.Precision.HIGHEST,
        )

    def some(step, carry):
        start = pl.multiple_of(step * group, group)
        query = arrived_ref[pl.ds(start, group), 0:tokens, :].reshape(wide, dim)
        out_ref[pl.ds(start, group), 0:rows] = against(
            query, lambda k, j: store_ref[k, j], tokens, 1
        )
        return carry

    lax.fori_loop(0, slots // group, some, 0)
    query = arrived_ref[:, tokens:height, :].reshape(wide, dim)
    out_ref[:, rows : 2 * rows] = against(
        query, lambda k, j: hot_refs[k][j], extra, -1
    )


def score(seat, arrived, store, hot_parts):
    count, height, dim = arrived.shape
    _, part, length, _ = store.shape
    rows = PLANE * part
    slots = 32
    hot_spec = pl.BlockSpec((part, length, dim), lambda i: (0, 0, 0))
    return pl.pallas_call(
        score_kernel,
        name="score",
        grid=(count // slots,),
        out_shape=jax.ShapeDtypeStruct((count, 2 * rows), F32),
        in_specs=[
            smem(),
            pl.BlockSpec((slots, height, dim), lambda i: (i, 0, 0)),
            pl.BlockSpec((PLANE, part, length, dim), lambda i: (0, 0, 0, 0)),
        ] + [hot_spec] * PLANE,
        out_specs=pl.BlockSpec((slots, 2 * rows), lambda i: (i, 0)),
        scratch_shapes=[pltpu.VMEM((rows, 8, 256), F32)],
        cost_estimate=cost(
            2 * count * height * rows * length * dim,
            2 * (count * height + 2 * rows * length) * dim,
        ),
    )(seat, arrived, store, *hot_parts)


def finish_kernel(note_ref, holder_ref, row_ref, back_ref, out_ref):
    queries, slots = holder_ref.shape
    device_count, wide = back_ref.shape
    rows = wide // 2
    busiest = note_ref[0]
    back = back_ref[...]
    near = back[:, :rows]
    first = near.astype(BF16)
    rest = near - first.astype(F32)
    second = rest.astype(BF16)
    third = (rest - second.astype(F32)).astype(BF16)
    device_iota = lax.broadcasted_iota(jnp.int32, (queries, device_count), 1)
    row_iota = lax.broadcasted_iota(jnp.int32, (queries, rows), 1)
    query_iota = lax.broadcasted_iota(jnp.int32, (queries, rows), 0)
    holder_all = holder_ref[...].astype(jnp.int32)
    row_all = row_ref[...].astype(jnp.int32)
    marks = [
        jnp.where(device_iota == holder_all[:, c : c + 1], 1.0, 0.0)
        for c in range(slots)
    ]
    mark = jnp.concatenate(marks, axis=0).astype(BF16)
    away = (
        jnp.dot(mark, first, preferred_element_type=F32)
        + jnp.dot(mark, second, preferred_element_type=F32)
    ) + jnp.dot(mark, third, preferred_element_type=F32)
    plane = pl.multiple_of(busiest // PLANE * PLANE, PLANE)
    parts = back_ref[pl.ds(plane, PLANE), :][:, rows:]
    half = PLANE // 2
    early = jnp.sum(parts[:half], axis=0, keepdims=True)
    later = jnp.sum(parts[half:], axis=0, keepdims=True)
    picked = []
    for c in range(slots):
        holder = holder_all[:, c : c + 1]
        found = away[c * queries : (c + 1) * queries]
        found = jnp.where(
            holder == busiest,
            jnp.where(
                query_iota == note_ref[1], early,
                jnp.where(query_iota == note_ref[2], later, found),
            ),
            found,
        )
        value = jnp.sum(
            jnp.where(row_iota == row_all[:, c : c + 1], found, 0.0),
            axis=1, keepdims=True,
        )
        picked.append(jnp.where(holder >= 0, value, 0.0))
    out_ref[...] = columns(picked, slots)


def finish(note, holder, row, back):
    return pl.pallas_call(
        finish_kernel,
        name="finish",
        out_shape=jax.ShapeDtypeStruct(holder.shape, F32),
        in_specs=[smem(), vmem(), vmem(), vmem()],
        out_specs=vmem(),
    )(note, holder, row, back)


def turn(value, hop, planes):
    pairs = [
        (p * PLANE + s, p * PLANE + (s + hop) % PLANE)
        for p in range(planes) for s in range(PLANE)
    ]
    return lax.ppermute(value, "shard", pairs)


def local(
    query_tokens, candidates, cand_count, placement_map,
    passage_base, residual_codes, passage_lengths, bucket_weights,
):
    device_count = lax.axis_size("shard")
    planes = device_count // PLANE
    seat = lax.rem(lax.axis_index("shard"), PLANE).astype(jnp.int32).reshape(1)
    store_rows = passage_base.shape[0]
    store = decode(seat, passage_base, residual_codes, passage_lengths, bucket_weights)
    parts = [store[0]] + [turn(store[k], k, planes) for k in range(1, PLANE)]
    outgoing, holder, row, note = prepare(
        candidates, cand_count, placement_map, query_tokens, store_rows, device_count
    )
    arrived = lax.all_to_all(outgoing, "shard", 0, 0, tiled=True)
    wanted = lax.rem(seat[0] - lax.rem(note[0], PLANE) + PLANE, PLANE)
    piece = parts[0]
    for k in range(1, PLANE):
        piece = jnp.where(wanted == k, parts[k], piece)
    hot_parts = [piece] + [turn(piece, k, planes) for k in range(1, PLANE)]
    visited = score(seat, arrived, store, hot_parts)
    back = lax.all_to_all(visited, "shard", 0, 0, tiled=True)
    return finish(note, holder, row, back)


def solution(mesh):
    whole = P(("groups", "shard"))
    return jax.shard_map(
        local,
        mesh=mesh,
        in_specs=(whole, whole, whole, P("groups"), whole, whole, whole, P("groups")),
        out_specs=whole,
        check_vma=False,
    )
```

```python
import functools

import jax
import jax.numpy as jnp
from jax import lax
from jax.experimental import pallas as pl
from jax.experimental.pallas import tpu as pltpu
from jax.sharding import PartitionSpec as P

EPSILON = 1e-06
PLANE = 8
F32 = jnp.float32
BF16 = jnp.bfloat16


def vmem(*_):
    return pl.BlockSpec(memory_space=pltpu.VMEM)


def near(value):
    return pltpu.with_memory_space_constraint(value, pltpu.VMEM)


def smem(*_):
    return pl.BlockSpec(memory_space=pltpu.SMEM)


def cost(flops, moved):
    return pl.CostEstimate(flops=flops, transcendentals=0, bytes_accessed=moved)


def log2(value):
    assert value & (value - 1) == 0
    return value.bit_length() - 1


def prepare_kernel(
    store_rows, device_count,
    cand_ref, count_ref, map_ref, query_ref,
    out_ref, holder_ref, row_ref, turned_ref, note_ref,
    present_ref, pick_vmem, pick_smem, sem,
):
    slots, queries = cand_ref.shape
    table_rows, lanes = map_ref.shape
    groups = lanes // queries
    per = slots // groups
    part_bits = log2(store_rows // PLANE)
    table = map_ref[...]
    holder_table = lax.shift_right_logical(table, log2(store_rows))
    row_table = table & (store_rows - 1)
    both = jnp.concatenate([holder_table, row_table], axis=1).astype(F32)
    both = jnp.transpose(both).astype(BF16)
    ids = cand_ref[...]
    ids = jnp.concatenate([ids[g * per : (g + 1) * per] for g in range(groups)], axis=1)
    count = jnp.concatenate([count_ref[...]] * groups, axis=1)
    high = lax.shift_right_logical(ids, log2(lanes))
    low = ids & (lanes - 1)
    lane = lax.broadcasted_iota(jnp.int32, (1, lanes), 1)
    first_slot = lax.shift_right_logical(lane, log2(queries)) * per
    table_iota = lax.broadcasted_iota(jnp.int32, (table_rows, lanes), 0)
    low_iota = lax.broadcasted_iota(jnp.int32, (lanes, lanes), 0)
    device_iota = lax.broadcasted_iota(jnp.int32, (device_count, lanes), 0)
    present = jnp.zeros((device_count, lanes), F32)
    for s in range(per):
        mark = jnp.where(table_iota == high[s : s + 1], 1.0, 0.0).astype(BF16)
        got = jnp.dot(both, mark, preferred_element_type=F32)
        here = low_iota == low[s : s + 1]
        holder = jnp.sum(jnp.where(here, got[:lanes], 0.0), axis=0, keepdims=True)
        row = jnp.sum(jnp.where(here, got[lanes:], 0.0), axis=0, keepdims=True)
        row = row.astype(jnp.int32)
        holder = jnp.where(first_slot + s < count, holder.astype(jnp.int32), -1)
        present = jnp.where(device_iota == holder, 1.0, present)
        block = (lax.shift_right_logical(row, part_bits) - holder) & (PLANE - 1)
        holder_ref[s : s + 1] = holder
        row_ref[s : s + 1] = row
        turned_ref[s : s + 1] = (block << part_bits) + (row & ((1 << part_bits) - 1))
    shift = queries
    while shift < lanes:
        present = jnp.maximum(present, pltpu.roll(present, shift, 1))
        shift *= 2
    present = jnp.where(lane < queries, present, 0.0)
    present_ref[...] = present
    kind = lax.broadcasted_iota(jnp.int32, (16, lanes), 0)
    lane_all = lax.broadcasted_iota(jnp.int32, (16, lanes), 1)
    weigh = jnp.where(kind == 0, lane_all, jnp.where(kind == 1, 1, 0))
    sums = lax.dot_general(
        weigh.astype(F32).astype(BF16), present.astype(BF16),
        (((1,), (1,)), ((), ())), preferred_element_type=F32,
    )
    device = lax.broadcasted_iota(jnp.int32, (1, device_count), 1)
    busiest = jnp.max(jnp.where(sums[1:2] > 1.5, device.astype(F32), 0.0)).astype(jnp.int32)
    theirs = present_ref[pl.ds(busiest, 1), :]
    lane_f = lane.astype(F32)
    last = jnp.max(theirs * lane_f).astype(jnp.int32)
    first = queries - 1 - jnp.max(theirs * (queries - 1 - lane_f)).astype(jnp.int32)
    middle = jnp.sum(theirs * lane_f).astype(jnp.int32) - first - last
    middle = jnp.clip(middle, 0, queries - 1)
    pick = jnp.where(device == busiest, last, sums[0:1].astype(jnp.int32))
    pick_vmem[...] = jnp.clip(pick, 0, queries - 1)
    copy = pltpu.make_async_copy(pick_vmem, pick_smem, sem)
    copy.start()
    note_ref[0] = busiest
    note_ref[1] = first
    note_ref[2] = middle
    note_ref[3] = last
    tokens = query_ref.shape[1]
    extra = 2 * tokens // PLANE
    spare = []
    for seat in range(PLANE):
        query = first if seat < PLANE // 2 else middle
        start = (seat % (PLANE // 2)) * extra
        spare.append(query_ref[query, start : start + extra, :])
    copy.wait()

    def pack(step, carry):
        for seat in range(PLANE):
            device = step * PLANE + seat
            out_ref[device, 0:tokens, :] = query_ref[pick_smem[0, device]]
            out_ref[device, tokens : tokens + extra, :] = spare[seat]
        return carry

    lax.fori_loop(0, device_count // PLANE, pack, 0)


def prepare(candidates, cand_count, placement_map, query_tokens, store_rows, device_count):
    queries, slots = candidates.shape
    _, tokens, dim = query_tokens.shape
    wide = jax.ShapeDtypeStruct((slots * queries // dim, dim), jnp.int32)
    return pl.pallas_call(
        functools.partial(prepare_kernel, store_rows, device_count),
        name="prepare",
        out_shape=(
            jax.ShapeDtypeStruct((device_count, tokens + 2 * tokens // PLANE, dim), BF16),
            wide, wide, wide,
            jax.ShapeDtypeStruct((4,), jnp.int32),
        ),
        in_specs=[vmem(), vmem(), vmem(), vmem()],
        out_specs=(vmem(), vmem(), vmem(), vmem(), smem()),
        scratch_shapes=[
            pltpu.VMEM((device_count, dim), F32),
            pltpu.VMEM((1, device_count), jnp.int32),
            pltpu.SMEM((1, device_count), jnp.int32),
            pltpu.SemaphoreType.DMA(()),
        ],
        cost_estimate=cost(10**9, 2 * 10**6),
    )(
        jnp.transpose(candidates),
        cand_count.reshape(1, queries),
        placement_map.reshape(-1, dim),
        query_tokens,
    )


def decode_kernel(seat_ref, length_ref, level_ref, base_ref, code_ref, out_ref):
    part, length, dim = base_ref.shape
    block = lax.rem(seat_ref[0] + pl.program_id(0), PLANE)
    token = lax.broadcasted_iota(jnp.int32, (length, dim), 0)
    for index in range(part):
        code = code_ref[index]
        residual = jnp.where(
            code < 2,
            jnp.where(code == 0, level_ref[0], level_ref[1]),
            jnp.where(code == 2, level_ref[2], level_ref[3]),
        )
        summed = base_ref[index].astype(F32) + residual
        inverse = lax.rsqrt(jnp.sum(summed * summed, axis=1, keepdims=True) + EPSILON)
        tokens = summed * inverse
        tokens = jnp.where(token < length_ref[block * part + index], tokens, tokens[0:1])
        out_ref[0, index] = tokens.astype(BF16)


def decode(seat, passage_base, residual_codes, passage_lengths, bucket_weights):
    rows, length, dim = passage_base.shape
    part = rows // PLANE
    spec = pl.BlockSpec(
        (part, length, dim), lambda i, seat_ref: (lax.rem(seat_ref[0] + i, PLANE), 0, 0)
    )
    return pl.pallas_call(
        decode_kernel,
        name="decode",
        out_shape=jax.ShapeDtypeStruct((PLANE, part, length, dim), BF16),
        grid_spec=pltpu.PrefetchScalarGridSpec(
            num_scalar_prefetch=1,
            grid=(PLANE,),
            in_specs=[smem(), smem(), spec, spec],
            out_specs=pl.BlockSpec((1, part, length, dim), lambda i, _: (i, 0, 0, 0)),
        ),
        cost_estimate=cost(rows * length * dim * 20, rows * length * dim * 8),
    )(seat, passage_lengths, bucket_weights, passage_base, residual_codes)


def score_kernel(arrived_ref, store_ref, *refs):
    hot_refs, (out_ref,) = refs[:PLANE], refs[PLANE:]
    count, height, dim = arrived_ref.shape
    _, part, length, _ = store_ref.shape
    rows = PLANE * part
    tokens = height * PLANE // (PLANE + 2)
    extra = height - tokens
    group = 256 // tokens
    slots = 256 // extra
    wide = 256

    def against(query, block, span):
        best = []
        for row in range(rows):
            similar = lax.dot_general(
                block(row // part, row % part), query, (((1,), (1,)), ((), ())),
                preferred_element_type=F32,
            )
            best.append(jnp.max(similar, axis=0, keepdims=True))
        best = jnp.concatenate(best, axis=0)
        first = best.astype(BF16)
        rest = best - first.astype(F32)
        second = rest.astype(BF16)
        third = (rest - second.astype(F32)).astype(BF16)
        member = lax.broadcasted_iota(jnp.int32, (wide // span, wide), 1) // span
        mine = lax.broadcasted_iota(jnp.int32, (wide // span, wide), 0)
        picks = jnp.where(member == mine, 1.0, 0.0).astype(BF16)
        total = [
            lax.dot_general(
                picks, piece, (((1,), (1,)), ((), ())), preferred_element_type=F32
            )
            for piece in (first, second, third)
        ]
        return (total[0] + total[1]) + total[2]

    def some(step, carry):
        start = pl.multiple_of(step * slots, slots)
        for inner in range(slots // group):
            here = pl.ds(start + inner * group, group)
            query = arrived_ref[here, 0:tokens, :].reshape(wide, dim)
            out_ref[here, 0:rows] = against(query, lambda k, j: store_ref[k, j], tokens)
        here = pl.ds(start, slots)
        query = arrived_ref[here, tokens:height, :].reshape(wide, dim)
        out_ref[here, rows : 2 * rows] = against(query, lambda k, j: hot_refs[k][j], extra)
        return carry

    lax.fori_loop(0, count // slots, some, 0)


def score(arrived, store, hot_parts):
    count, height, dim = arrived.shape
    _, part, length, _ = store.shape
    rows = PLANE * part
    return pl.pallas_call(
        score_kernel,
        name="score",
        compiler_params=pltpu.CompilerParams(vmem_limit_bytes=16 * 2**20),
        out_shape=pltpu.VMEM((count, 2 * rows), F32),
        in_specs=[vmem()] * (2 + PLANE),
        out_specs=vmem(),
        cost_estimate=cost(
            2 * count * height * rows * length * dim,
            2 * (count * height + 2 * rows * length) * dim,
        ),
    )(near(arrived), store, *[near(part) for part in hot_parts])


def finish_kernel(note_ref, holder_ref, row_ref, turned_ref, back_ref, out_ref):
    slots, queries = out_ref.shape
    per, lanes = holder_ref.shape
    device_count, double = back_ref.shape
    rows = double // 2
    part = rows // PLANE
    busiest = note_ref[0]
    back = jnp.transpose(back_ref[...])
    near, far = back[:rows], back[rows:]
    first = near.astype(BF16)
    rest = near - first.astype(F32)
    second = rest.astype(BF16)
    third = (rest - second.astype(F32)).astype(BF16)
    pieces = jnp.concatenate([first, second, third], axis=0)
    device_iota = lax.broadcasted_iota(jnp.int32, (device_count, lanes), 0)
    row_iota = lax.broadcasted_iota(jnp.int32, (rows, lanes), 0)
    lane = lax.broadcasted_iota(jnp.int32, (1, lanes), 1)
    query = lane & (queries - 1)
    device_lane = lax.broadcasted_iota(jnp.int32, (rows, device_count), 1)
    plane = busiest - lax.rem(busiest, PLANE)
    sums = []
    for half in range(2):
        total = jnp.zeros((rows, 1), F32)
        for seat in range(half * PLANE // 2, (half + 1) * PLANE // 2):
            mine = jnp.sum(
                jnp.where(device_lane == plane + seat, far, 0.0), axis=1, keepdims=True
            )
            if seat:
                cut = rows - seat * part
                mine = jnp.concatenate([mine[cut:], mine[:cut]], axis=0)
            total = total + mine
        sums.append(total)
    values = []
    for s in range(per):
        holder = holder_ref[s : s + 1]
        mark = jnp.where(device_iota == holder, 1.0, 0.0).astype(BF16)
        three = jnp.dot(pieces, mark, preferred_element_type=F32)
        away = (three[:rows] + three[rows : 2 * rows]) + three[2 * rows :]
        hot = (holder == busiest) & ((query == note_ref[1]) | (query == note_ref[2]))
        extra = jnp.where(query == note_ref[1], sums[0], sums[1])
        found = jnp.where(hot, extra, away)
        row = jnp.where(hot, row_ref[s : s + 1], turned_ref[s : s + 1])
        value = jnp.sum(jnp.where(row_iota == row, found, 0.0), axis=0, keepdims=True)
        values.append(jnp.where(holder >= 0, value, 0.0))
    values = jnp.concatenate(values, axis=0)
    for g in range(slots // per):
        out_ref[g * per : (g + 1) * per, :] = values[:, g * queries : (g + 1) * queries]


def finish(note, holder, row, turned, back, slots, queries):
    return pl.pallas_call(
        finish_kernel,
        name="finish",
        out_shape=jax.ShapeDtypeStruct((slots, queries), F32),
        in_specs=[smem(), vmem(), vmem(), vmem(), vmem()],
        out_specs=vmem(),
    )(note, holder, row, turned, near(back))


def turn(value, hop, planes):
    pairs = [
        (p * PLANE + s, p * PLANE + (s + hop) % PLANE)
        for p in range(planes) for s in range(PLANE)
    ]
    return lax.ppermute(value, "shard", pairs)


def local(
    query_tokens, candidates, cand_count, placement_map,
    passage_base, residual_codes, passage_lengths, bucket_weights,
):
    device_count = lax.axis_size("shard")
    planes = device_count // PLANE
    seat = lax.rem(lax.axis_index("shard"), PLANE).astype(jnp.int32).reshape(1)
    store_rows = passage_base.shape[0]
    store = decode(seat, passage_base, residual_codes, passage_lengths, bucket_weights)
    parts = [store[0]] + [turn(store[k], k, planes) for k in range(1, PLANE)]
    outgoing, holder, row, turned, note = prepare(
        candidates, cand_count, placement_map, query_tokens, store_rows, device_count
    )
    arrived = lax.all_to_all(outgoing, "shard", 0, 0, tiled=True)
    wanted = lax.rem(seat[0] - lax.rem(note[0], PLANE) + PLANE, PLANE)
    piece = parts[0]
    for k in range(1, PLANE):
        piece = jnp.where(wanted == k, parts[k], piece)
    hot_parts = [piece] + [turn(piece, -k, planes) for k in range(1, PLANE)]
    visited = score(arrived, store, hot_parts)
    back = lax.all_to_all(visited, "shard", 0, 0, tiled=True)
    queries, slots = candidates.shape
    return jnp.transpose(finish(note, holder, row, turned, back, slots, queries))


def solution(mesh):
    whole = P(("groups", "shard"))
    return jax.shard_map(
        local,
        mesh=mesh,
        in_specs=(whole, whole, whole, P("groups"), whole, whole, whole, P("groups")),
        out_specs=whole,
        check_vma=False,
    )
```

```python
import functools

import jax
import jax.numpy as jnp
from jax import lax
from jax.experimental import pallas as pl
from jax.experimental.pallas import tpu as pltpu
from jax.sharding import PartitionSpec as P

EPSILON = 1e-06
PLANE = 8
F32 = jnp.float32
BF16 = jnp.bfloat16


def vmem(*_):
    return pl.BlockSpec(memory_space=pltpu.VMEM)


def near(value):
    return pltpu.with_memory_space_constraint(value, pltpu.VMEM)


def smem(*_):
    return pl.BlockSpec(memory_space=pltpu.SMEM)


def cost(flops, moved):
    return pl.CostEstimate(flops=flops, transcendentals=0, bytes_accessed=moved)


def log2(value):
    assert value & (value - 1) == 0
    return value.bit_length() - 1


def prepare_kernel(
    store_rows, device_count,
    cand_ref, count_ref, map_ref, query_ref,
    out_ref, holder_ref, row_ref, turned_ref, note_ref,
    present_ref, pick_vmem, pick_smem, sem, tokens_ref, packed_ref, in_sem, out_sem,
):
    load = pltpu.make_async_copy(query_ref, tokens_ref, in_sem)
    load.start()
    slots, queries = cand_ref.shape
    table_rows, lanes = map_ref.shape
    groups = lanes // queries
    per = slots // groups
    part_bits = log2(store_rows // PLANE)
    table = map_ref[...]
    holder_table = lax.shift_right_logical(table, log2(store_rows))
    row_table = table & (store_rows - 1)
    both = jnp.concatenate([holder_table, row_table], axis=1).astype(F32)
    both = jnp.transpose(both).astype(BF16)
    ids = cand_ref[...]
    ids = jnp.concatenate([ids[g * per : (g + 1) * per] for g in range(groups)], axis=1)
    count = jnp.concatenate([count_ref[...]] * groups, axis=1)
    high = lax.shift_right_logical(ids, log2(lanes))
    low = ids & (lanes - 1)
    lane = lax.broadcasted_iota(jnp.int32, (1, lanes), 1)
    first_slot = lax.shift_right_logical(lane, log2(queries)) * per
    table_iota = lax.broadcasted_iota(jnp.int32, (table_rows, lanes), 0)
    low_iota = lax.broadcasted_iota(jnp.int32, (lanes, lanes), 0)
    device_iota = lax.broadcasted_iota(jnp.int32, (device_count, lanes), 0)
    present = jnp.zeros((device_count, lanes), F32)
    for s in range(per):
        mark = jnp.where(table_iota == high[s : s + 1], 1.0, 0.0).astype(BF16)
        got = jnp.dot(both, mark, preferred_element_type=F32)
        here = low_iota == low[s : s + 1]
        holder = jnp.sum(jnp.where(here, got[:lanes], 0.0), axis=0, keepdims=True)
        row = jnp.sum(jnp.where(here, got[lanes:], 0.0), axis=0, keepdims=True)
        row = row.astype(jnp.int32)
        holder = jnp.where(first_slot + s < count, holder.astype(jnp.int32), -1)
        present = jnp.where(device_iota == holder, 1.0, present)
        block = (lax.shift_right_logical(row, part_bits) - holder) & (PLANE - 1)
        holder_ref[s : s + 1] = holder
        row_ref[s : s + 1] = row
        turned_ref[s : s + 1] = (block << part_bits) + (row & ((1 << part_bits) - 1))
    shift = queries
    while shift < lanes:
        present = jnp.maximum(present, pltpu.roll(present, shift, 1))
        shift *= 2
    present = jnp.where(lane < queries, present, 0.0)
    present_ref[...] = present
    kind = lax.broadcasted_iota(jnp.int32, (16, lanes), 0)
    lane_all = lax.broadcasted_iota(jnp.int32, (16, lanes), 1)
    weigh = jnp.where(kind == 0, lane_all, jnp.where(kind == 1, 1, 0))
    sums = lax.dot_general(
        weigh.astype(F32).astype(BF16), present.astype(BF16),
        (((1,), (1,)), ((), ())), preferred_element_type=F32,
    )
    device = lax.broadcasted_iota(jnp.int32, (1, device_count), 1)
    busiest = jnp.max(jnp.where(sums[1:2] > 1.5, device.astype(F32), 0.0)).astype(jnp.int32)
    theirs = present_ref[pl.ds(busiest, 1), :]
    lane_f = lane.astype(F32)
    last = jnp.max(theirs * lane_f).astype(jnp.int32)
    first = queries - 1 - jnp.max(theirs * (queries - 1 - lane_f)).astype(jnp.int32)
    middle = jnp.sum(theirs * lane_f).astype(jnp.int32) - first - last
    middle = jnp.clip(middle, 0, queries - 1)
    pick = jnp.where(device == busiest, last, sums[0:1].astype(jnp.int32))
    pick_vmem[...] = jnp.clip(pick, 0, queries - 1)
    copy = pltpu.make_async_copy(pick_vmem, pick_smem, sem)
    copy.start()
    note_ref[0] = busiest
    note_ref[1] = first
    note_ref[2] = middle
    note_ref[3] = last
    tokens = query_ref.shape[1]
    extra = 2 * tokens // PLANE
    load.wait()
    spare = []
    for seat in range(PLANE):
        query = first if seat < PLANE // 2 else middle
        start = (seat % (PLANE // 2)) * extra
        spare.append(tokens_ref[query, start : start + extra, :])
    copy.wait()
    chunks = 4
    size = device_count // chunks
    stores = []
    for chunk in range(chunks):

        def pack(step, carry):
            for seat in range(PLANE):
                device = chunk * size + step * PLANE + seat
                packed_ref[device, 0:tokens, :] = tokens_ref[pick_smem[0, device]]
                packed_ref[device, tokens : tokens + extra, :] = spare[seat]
            return carry

        lax.fori_loop(0, size // PLANE, pack, 0)
        here = pl.ds(chunk * size, size)
        store = pltpu.make_async_copy(packed_ref.at[here], out_ref.at[here], out_sem.at[chunk])
        store.start()
        stores.append(store)
    for store in stores:
        store.wait()


def prepare(candidates, cand_count, placement_map, query_tokens, store_rows, device_count):
    queries, slots = candidates.shape
    _, tokens, dim = query_tokens.shape
    wide = jax.ShapeDtypeStruct((slots * queries // dim, dim), jnp.int32)
    return pl.pallas_call(
        functools.partial(prepare_kernel, store_rows, device_count),
        name="prepare",
        out_shape=(
            jax.ShapeDtypeStruct((device_count, tokens + 2 * tokens // PLANE, dim), BF16),
            wide, wide, wide,
            jax.ShapeDtypeStruct((4,), jnp.int32),
        ),
        in_specs=[vmem(), vmem(), vmem(), pl.BlockSpec(memory_space=pl.ANY)],
        out_specs=(pl.BlockSpec(memory_space=pl.ANY), vmem(), vmem(), vmem(), smem()),
        scratch_shapes=[
            pltpu.VMEM((device_count, dim), F32),
            pltpu.VMEM((1, device_count), jnp.int32),
            pltpu.SMEM((1, device_count), jnp.int32),
            pltpu.SemaphoreType.DMA(()),
            pltpu.VMEM((queries, tokens, dim), BF16),
            pltpu.VMEM((device_count, tokens + 2 * tokens // PLANE, dim), BF16),
            pltpu.SemaphoreType.DMA(()),
            pltpu.SemaphoreType.DMA((4,)),
        ],
        cost_estimate=cost(10**9, 2 * 10**6),
    )(
        jnp.transpose(candidates),
        cand_count.reshape(1, queries),
        placement_map.reshape(-1, dim),
        query_tokens,
    )


def decode_kernel(seat_ref, length_ref, level_ref, base_ref, code_ref, out_ref):
    part, length, dim = base_ref.shape
    block = lax.rem(seat_ref[0] + pl.program_id(0), PLANE)
    token = lax.broadcasted_iota(jnp.int32, (length, dim), 0)
    for index in range(part):
        code = code_ref[index]
        residual = jnp.where(
            code < 2,
            jnp.where(code == 0, level_ref[0], level_ref[1]),
            jnp.where(code == 2, level_ref[2], level_ref[3]),
        )
        summed = base_ref[index].astype(F32) + residual
        inverse = lax.rsqrt(jnp.sum(summed * summed, axis=1, keepdims=True) + EPSILON)
        tokens = summed * inverse
        tokens = jnp.where(token < length_ref[block * part + index], tokens, tokens[0:1])
        out_ref[0, index] = tokens.astype(BF16)


def decode(seat, passage_base, residual_codes, passage_lengths, bucket_weights):
    rows, length, dim = passage_base.shape
    part = rows // PLANE
    spec = pl.BlockSpec(
        (part, length, dim), lambda i, seat_ref: (lax.rem(seat_ref[0] + i, PLANE), 0, 0)
    )
    return pl.pallas_call(
        decode_kernel,
        name="decode",
        out_shape=jax.ShapeDtypeStruct((PLANE, part, length, dim), BF16),
        grid_spec=pltpu.PrefetchScalarGridSpec(
            num_scalar_prefetch=1,
            grid=(PLANE,),
            in_specs=[smem(), smem(), spec, spec],
            out_specs=pl.BlockSpec((1, part, length, dim), lambda i, _: (i, 0, 0, 0)),
        ),
        cost_estimate=cost(rows * length * dim * 20, rows * length * dim * 8),
    )(seat, passage_lengths, bucket_weights, passage_base, residual_codes)


def score_kernel(arrived_ref, store_ref, *refs):
    hot_refs, (out_ref, best_ref) = refs[:PLANE], refs[PLANE:]
    count, height, dim = arrived_ref.shape
    _, part, length, _ = store_ref.shape
    rows = PLANE * part
    tokens = height * PLANE // (PLANE + 2)
    extra = height - tokens
    group = 256 // tokens
    slots = 256 // extra
    wide = 256

    def against(index, query, block):
        best = []
        for row in range(rows):
            similar = lax.dot_general(
                block(row // part, row % part), query, (((1,), (1,)), ((), ())),
                preferred_element_type=F32,
            )
            best.append(jnp.max(similar, axis=0, keepdims=True))
        best_ref[index] = jnp.concatenate(best, axis=0)

    blocks = count // slots
    inner_blocks = slots // group

    def some(step, carry):
        start = pl.multiple_of(step * slots, slots)
        for inner in range(inner_blocks):
            here = pl.ds(start + inner * group, group)
            query = arrived_ref[here, 0:tokens, :].reshape(wide, dim)
            against(step * inner_blocks + inner, query, lambda k, j: store_ref[k, j])
        query = arrived_ref[pl.ds(start, slots), tokens:height, :].reshape(wide, dim)
        against(blocks * inner_blocks + step, query, lambda k, j: hot_refs[k][j])
        return carry

    lax.fori_loop(0, blocks, some, 0)
    slot = lax.broadcasted_iota(jnp.int32, (wide, count), 1)
    token = lax.broadcasted_iota(jnp.int32, (wide, count), 0)

    def sums(first_block, number, span):
        member = lax.shift_right_logical(token, log2(span))
        total = jnp.zeros((3 * rows, count), F32)
        for index in range(number):
            best = best_ref[first_block + index]
            first = best.astype(BF16)
            rest = best - first.astype(F32)
            second = rest.astype(BF16)
            third = (rest - second.astype(F32)).astype(BF16)
            picks = jnp.where(slot == member + index * (wide // span), 1.0, 0.0).astype(BF16)
            total = total + jnp.dot(
                jnp.concatenate([first, second, third], axis=0), picks,
                preferred_element_type=F32,
            )
        return (total[:rows] + total[rows : 2 * rows]) + total[2 * rows :]

    near_sums = sums(0, blocks * inner_blocks, tokens)
    far_sums = sums(blocks * inner_blocks, blocks, extra)
    out_ref[...] = jnp.transpose(jnp.concatenate([near_sums, far_sums], axis=0))


def score(arrived, store, hot_parts):
    count, height, dim = arrived.shape
    _, part, length, _ = store.shape
    rows = PLANE * part
    return pl.pallas_call(
        score_kernel,
        name="score",
        compiler_params=pltpu.CompilerParams(vmem_limit_bytes=16 * 2**20),
        out_shape=pltpu.VMEM((count, 2 * rows), F32),
        in_specs=[vmem()] * (2 + PLANE),
        out_specs=vmem(),
        scratch_shapes=[pltpu.VMEM((count * height // 256, rows, 256), F32)],
        cost_estimate=cost(
            2 * count * height * rows * length * dim,
            2 * (count * height + 2 * rows * length) * dim,
        ),
    )(near(arrived), store, *[near(part) for part in hot_parts])


def finish_kernel(note_ref, holder_ref, row_ref, turned_ref, back_ref, out_ref):
    slots, queries = out_ref.shape
    per, lanes = holder_ref.shape
    device_count, double = back_ref.shape
    rows = double // 2
    part = rows // PLANE
    busiest = note_ref[0]
    back = jnp.transpose(back_ref[...])
    near, far = back[:rows], back[rows:]
    first = near.astype(BF16)
    rest = near - first.astype(F32)
    second = rest.astype(BF16)
    third = (rest - second.astype(F32)).astype(BF16)
    pieces = jnp.concatenate([first, second, third], axis=0)
    device_iota = lax.broadcasted_iota(jnp.int32, (device_count, lanes), 0)
    row_iota = lax.broadcasted_iota(jnp.int32, (rows, lanes), 0)
    lane = lax.broadcasted_iota(jnp.int32, (1, lanes), 1)
    query = lane & (queries - 1)
    device_lane = lax.broadcasted_iota(jnp.int32, (rows, device_count), 1)
    plane = busiest - lax.rem(busiest, PLANE)
    sums = []
    for half in range(2):
        total = jnp.zeros((rows, 1), F32)
        for seat in range(half * PLANE // 2, (half + 1) * PLANE // 2):
            mine = jnp.sum(
                jnp.where(device_lane == plane + seat, far, 0.0), axis=1, keepdims=True
            )
            if seat:
                cut = rows - seat * part
                mine = jnp.concatenate([mine[cut:], mine[:cut]], axis=0)
            total = total + mine
        sums.append(total)
    values = []
    for s in range(per):
        holder = holder_ref[s : s + 1]
        mark = jnp.where(device_iota == holder, 1.0, 0.0).astype(BF16)
        three = jnp.dot(pieces, mark, preferred_element_type=F32)
        away = (three[:rows] + three[rows : 2 * rows]) + three[2 * rows :]
        hot = (holder == busiest) & ((query == note_ref[1]) | (query == note_ref[2]))
        extra = jnp.where(query == note_ref[1], sums[0], sums[1])
        found = jnp.where(hot, extra, away)
        row = jnp.where(hot, row_ref[s : s + 1], turned_ref[s : s + 1])
        value = jnp.sum(jnp.where(row_iota == row, found, 0.0), axis=0, keepdims=True)
        values.append(jnp.where(holder >= 0, value, 0.0))
    values = jnp.concatenate(values, axis=0)
    for g in range(slots // per):
        out_ref[g * per : (g + 1) * per, :] = values[:, g * queries : (g + 1) * queries]


def finish(note, holder, row, turned, back, slots, queries):
    return pl.pallas_call(
        finish_kernel,
        name="finish",
        out_shape=jax.ShapeDtypeStruct((slots, queries), F32),
        in_specs=[smem(), vmem(), vmem(), vmem(), vmem()],
        out_specs=vmem(),
    )(note, near(holder), near(row), near(turned), near(back))


def turn(value, hop, planes):
    pairs = [
        (p * PLANE + s, p * PLANE + (s + hop) % PLANE)
        for p in range(planes) for s in range(PLANE)
    ]
    return lax.ppermute(value, "shard", pairs)


def local(
    query_tokens, candidates, cand_count, placement_map,
    passage_base, residual_codes, passage_lengths, bucket_weights,
):
    device_count = lax.axis_size("shard")
    planes = device_count // PLANE
    seat = lax.rem(lax.axis_index("shard"), PLANE).astype(jnp.int32).reshape(1)
    store_rows = passage_base.shape[0]
    store = decode(seat, passage_base, residual_codes, passage_lengths, bucket_weights)
    parts = [store[0]] + [turn(store[k], k, planes) for k in range(1, PLANE)]
    outgoing, holder, row, turned, note = prepare(
        candidates, cand_count, placement_map, query_tokens, store_rows, device_count
    )
    arrived = lax.all_to_all(outgoing, "shard", 0, 0, tiled=True)
    wanted = lax.rem(seat[0] - lax.rem(note[0], PLANE) + PLANE, PLANE)
    piece = parts[0]
    for k in range(1, PLANE):
        piece = jnp.where(wanted == k, parts[k], piece)
    hot_parts = [piece] + [turn(piece, -k, planes) for k in range(1, PLANE)]
    visited = score(arrived, store, hot_parts)
    back = lax.all_to_all(visited, "shard", 0, 0, tiled=True)
    queries, slots = candidates.shape
    return jnp.transpose(finish(note, holder, row, turned, back, slots, queries))


def solution(mesh):
    whole = P(("groups", "shard"))
    return jax.shard_map(
        local,
        mesh=mesh,
        in_specs=(whole, whole, whole, P("groups"), whole, whole, whole, P("groups")),
        out_specs=whole,
        check_vma=False,
    )
```

```python
import functools

import jax
import jax.numpy as jnp
from jax import lax
from jax.experimental import pallas as pl
from jax.experimental.pallas import tpu as pltpu
from jax.sharding import PartitionSpec as P

EPSILON = 1e-06
PLANE = 8
F32 = jnp.float32
BF16 = jnp.bfloat16


def vmem(*_):
    return pl.BlockSpec(memory_space=pltpu.VMEM)


def near(value):
    return pltpu.with_memory_space_constraint(value, pltpu.VMEM)


def smem(*_):
    return pl.BlockSpec(memory_space=pltpu.SMEM)


def cost(flops, moved):
    return pl.CostEstimate(flops=flops, transcendentals=0, bytes_accessed=moved)


def log2(value):
    assert value & (value - 1) == 0
    return value.bit_length() - 1


def prepare_kernel(
    store_rows, device_count,
    cand_ref, count_ref, map_ref, query_ref,
    out_ref, holder_ref, row_ref, turned_ref, note_ref, busiest_ref,
    present_ref, pick_vmem, pick_smem, sem, tokens_ref, packed_ref, in_sem, out_sem,
):
    load = pltpu.make_async_copy(query_ref, tokens_ref, in_sem)
    load.start()
    slots, queries = cand_ref.shape
    table_rows, lanes = map_ref.shape
    groups = lanes // queries
    per = slots // groups
    part_bits = log2(store_rows // PLANE)
    table = map_ref[...]
    holder_table = lax.shift_right_logical(table, log2(store_rows))
    row_table = table & (store_rows - 1)
    both = jnp.concatenate([holder_table, row_table], axis=1).astype(F32)
    both = jnp.transpose(both).astype(BF16)
    ids = cand_ref[...]
    ids = jnp.concatenate([ids[g * per : (g + 1) * per] for g in range(groups)], axis=1)
    count = jnp.concatenate([count_ref[...]] * groups, axis=1)
    high = lax.shift_right_logical(ids, log2(lanes))
    low = ids & (lanes - 1)
    lane = lax.broadcasted_iota(jnp.int32, (1, lanes), 1)
    first_slot = lax.shift_right_logical(lane, log2(queries)) * per
    table_iota = lax.broadcasted_iota(jnp.int32, (table_rows, lanes), 0)
    low_iota = lax.broadcasted_iota(jnp.int32, (lanes, lanes), 0)
    device_iota = lax.broadcasted_iota(jnp.int32, (device_count, lanes), 0)
    present = jnp.zeros((device_count, lanes), F32)
    for s in range(per):
        mark = jnp.where(table_iota == high[s : s + 1], 1.0, 0.0).astype(BF16)
        got = jnp.dot(both, mark, preferred_element_type=F32)
        here = low_iota == low[s : s + 1]
        holder = jnp.sum(jnp.where(here, got[:lanes], 0.0), axis=0, keepdims=True)
        row = jnp.sum(jnp.where(here, got[lanes:], 0.0), axis=0, keepdims=True)
        row = row.astype(jnp.int32)
        holder = jnp.where(first_slot + s < count, holder.astype(jnp.int32), -1)
        present = jnp.where(device_iota == holder, 1.0, present)
        block = (lax.shift_right_logical(row, part_bits) - holder) & (PLANE - 1)
        holder_ref[s : s + 1] = holder
        row_ref[s : s + 1] = row
        turned_ref[s : s + 1] = (block << part_bits) + (row & ((1 << part_bits) - 1))
    shift = queries
    while shift < lanes:
        present = jnp.maximum(present, pltpu.roll(present, shift, 1))
        shift *= 2
    present = jnp.where(lane < queries, present, 0.0)
    present_ref[...] = present
    kind = lax.broadcasted_iota(jnp.int32, (16, lanes), 0)
    lane_all = lax.broadcasted_iota(jnp.int32, (16, lanes), 1)
    weigh = jnp.where(kind == 0, lane_all, jnp.where(kind == 1, 1, 0))
    sums = lax.dot_general(
        weigh.astype(F32).astype(BF16), present.astype(BF16),
        (((1,), (1,)), ((), ())), preferred_element_type=F32,
    )
    device = lax.broadcasted_iota(jnp.int32, (1, device_count), 1)
    busiest = jnp.max(jnp.where(sums[1:2] > 1.5, device.astype(F32), 0.0)).astype(jnp.int32)
    theirs = present_ref[pl.ds(busiest, 1), :]
    lane_f = lane.astype(F32)
    last = jnp.max(theirs * lane_f).astype(jnp.int32)
    first = queries - 1 - jnp.max(theirs * (queries - 1 - lane_f)).astype(jnp.int32)
    middle = jnp.sum(theirs * lane_f).astype(jnp.int32) - first - last
    middle = jnp.clip(middle, 0, queries - 1)
    pick = jnp.where(device == busiest, last, sums[0:1].astype(jnp.int32))
    pick_vmem[...] = jnp.clip(pick, 0, queries - 1)
    copy = pltpu.make_async_copy(pick_vmem, pick_smem, sem)
    copy.start()
    busiest_ref[0] = busiest
    kind = lax.broadcasted_iota(jnp.int32, (8, device_count), 0)
    note_ref[...] = jnp.where(kind == 0, busiest, jnp.where(kind == 1, first, middle))
    tokens = query_ref.shape[1]
    extra = 2 * tokens // PLANE
    load.wait()
    spare = []
    for seat in range(PLANE):
        query = first if seat < PLANE // 2 else middle
        start = (seat % (PLANE // 2)) * extra
        spare.append(tokens_ref[query, start : start + extra, :])
    copy.wait()
    chunks = 4
    size = device_count // chunks
    stores = []
    for chunk in range(chunks):

        def pack(step, carry):
            for seat in range(PLANE):
                device = chunk * size + step * PLANE + seat
                packed_ref[device, 0:tokens, :] = tokens_ref[pick_smem[0, device]]
                packed_ref[device, tokens : tokens + extra, :] = spare[seat]
            return carry

        lax.fori_loop(0, size // PLANE, pack, 0)
        here = pl.ds(chunk * size, size)
        store = pltpu.make_async_copy(packed_ref.at[here], out_ref.at[here], out_sem.at[chunk])
        store.start()
        stores.append(store)
    for store in stores:
        store.wait()


def prepare(candidates, cand_count, placement_map, query_tokens, store_rows, device_count):
    queries, slots = candidates.shape
    _, tokens, dim = query_tokens.shape
    wide = pltpu.VMEM((slots * queries // dim, dim), jnp.int32)
    return pl.pallas_call(
        functools.partial(prepare_kernel, store_rows, device_count),
        name="prepare",
        out_shape=(
            jax.ShapeDtypeStruct((device_count, tokens + 2 * tokens // PLANE, dim), BF16),
            wide, wide, wide,
            pltpu.VMEM((8, device_count), jnp.int32),
            jax.ShapeDtypeStruct((1,), jnp.int32),
        ),
        in_specs=[vmem(), vmem(), vmem(), pl.BlockSpec(memory_space=pl.ANY)],
        out_specs=(pl.BlockSpec(memory_space=pl.ANY), vmem(), vmem(), vmem(), vmem(), smem()),
        scratch_shapes=[
            pltpu.VMEM((device_count, dim), F32),
            pltpu.VMEM((1, device_count), jnp.int32),
            pltpu.SMEM((1, device_count), jnp.int32),
            pltpu.SemaphoreType.DMA(()),
            pltpu.VMEM((queries, tokens, dim), BF16),
            pltpu.VMEM((device_count, tokens + 2 * tokens // PLANE, dim), BF16),
            pltpu.SemaphoreType.DMA(()),
            pltpu.SemaphoreType.DMA((4,)),
        ],
        cost_estimate=cost(10**9, 2 * 10**6),
    )(
        jnp.transpose(candidates),
        cand_count.reshape(1, queries),
        placement_map.reshape(-1, dim),
        query_tokens,
    )


def decode_kernel(seat_ref, length_ref, level_ref, base_ref, code_ref, out_ref):
    part, length, dim = base_ref.shape
    block = lax.rem(seat_ref[0] + pl.program_id(0), PLANE)
    token = lax.broadcasted_iota(jnp.int32, (length, dim), 0)
    for index in range(part):
        code = code_ref[index]
        residual = jnp.where(
            code < 2,
            jnp.where(code == 0, level_ref[0], level_ref[1]),
            jnp.where(code == 2, level_ref[2], level_ref[3]),
        )
        summed = base_ref[index].astype(F32) + residual
        inverse = lax.rsqrt(jnp.sum(summed * summed, axis=1, keepdims=True) + EPSILON)
        tokens = summed * inverse
        tokens = jnp.where(token < length_ref[block * part + index], tokens, tokens[0:1])
        out_ref[0, index] = tokens.astype(BF16)


def decode(seat, passage_base, residual_codes, passage_lengths, bucket_weights):
    rows, length, dim = passage_base.shape
    part = rows // PLANE
    spec = pl.BlockSpec(
        (part, length, dim), lambda i, seat_ref: (lax.rem(seat_ref[0] + i, PLANE), 0, 0)
    )
    return pl.pallas_call(
        decode_kernel,
        name="decode",
        out_shape=jax.ShapeDtypeStruct((PLANE, part, length, dim), BF16),
        grid_spec=pltpu.PrefetchScalarGridSpec(
            num_scalar_prefetch=1,
            grid=(PLANE,),
            in_specs=[smem(), smem(), spec, spec],
            out_specs=pl.BlockSpec((1, part, length, dim), lambda i, _: (i, 0, 0, 0)),
        ),
        cost_estimate=cost(rows * length * dim * 20, rows * length * dim * 8),
    )(seat, passage_lengths, bucket_weights, passage_base, residual_codes)


def score_kernel(arrived_ref, store_ref, *refs):
    hot_refs, (out_ref, best_ref) = refs[:PLANE], refs[PLANE:]
    count, height, dim = arrived_ref.shape
    _, part, length, _ = store_ref.shape
    rows = PLANE * part
    tokens = height * PLANE // (PLANE + 2)
    extra = height - tokens
    group = 256 // tokens
    slots = 256 // extra
    wide = 256

    def against(index, query, block):
        best = []
        for row in range(rows):
            similar = lax.dot_general(
                block(row // part, row % part), query, (((1,), (1,)), ((), ())),
                preferred_element_type=F32,
            )
            best.append(jnp.max(similar, axis=0, keepdims=True))
        best_ref[index] = jnp.concatenate(best, axis=0)

    blocks = count // slots
    inner_blocks = slots // group

    def some(step, carry):
        start = pl.multiple_of(step * slots, slots)
        for inner in range(inner_blocks):
            here = pl.ds(start + inner * group, group)
            query = arrived_ref[here, 0:tokens, :].reshape(wide, dim)
            against(step * inner_blocks + inner, query, lambda k, j: store_ref[k, j])
        query = arrived_ref[pl.ds(start, slots), tokens:height, :].reshape(wide, dim)
        against(blocks * inner_blocks + step, query, lambda k, j: hot_refs[k][j])
        return carry

    lax.fori_loop(0, blocks, some, 0)
    slot = lax.broadcasted_iota(jnp.int32, (wide, count), 1)
    token = lax.broadcasted_iota(jnp.int32, (wide, count), 0)

    def sums(first_block, number, span):
        member = lax.shift_right_logical(token, log2(span))
        total = jnp.zeros((3 * rows, count), F32)
        for index in range(number):
            best = best_ref[first_block + index]
            first = best.astype(BF16)
            rest = best - first.astype(F32)
            second = rest.astype(BF16)
            third = (rest - second.astype(F32)).astype(BF16)
            picks = jnp.where(slot == member + index * (wide // span), 1.0, 0.0).astype(BF16)
            total = total + jnp.dot(
                jnp.concatenate([first, second, third], axis=0), picks,
                preferred_element_type=F32,
            )
        return (total[:rows] + total[rows : 2 * rows]) + total[2 * rows :]

    near_sums = sums(0, blocks * inner_blocks, tokens)
    far_sums = sums(blocks * inner_blocks, blocks, extra)
    out_ref[...] = jnp.transpose(jnp.concatenate([near_sums, far_sums], axis=0))


def score(arrived, store, hot_parts):
    count, height, dim = arrived.shape
    _, part, length, _ = store.shape
    rows = PLANE * part
    return pl.pallas_call(
        score_kernel,
        name="score",
        compiler_params=pltpu.CompilerParams(vmem_limit_bytes=16 * 2**20),
        out_shape=pltpu.VMEM((count, 2 * rows), F32),
        in_specs=[vmem()] * (2 + PLANE),
        out_specs=vmem(),
        scratch_shapes=[pltpu.VMEM((count * height // 256, rows, 256), F32)],
        cost_estimate=cost(
            2 * count * height * rows * length * dim,
            2 * (count * height + 2 * rows * length) * dim,
        ),
    )(near(arrived), store, *[near(part) for part in hot_parts])


def finish_kernel(note_ref, holder_ref, row_ref, turned_ref, back_ref, out_ref):
    slots, queries = out_ref.shape
    per, lanes = holder_ref.shape
    device_count, double = back_ref.shape
    rows = double // 2
    part = rows // PLANE
    busiest = note_ref[0:1]
    first_hot = note_ref[1:2]
    second_hot = note_ref[2:3]
    back = jnp.transpose(back_ref[...])
    near, far = back[:rows], back[rows:]
    first = near.astype(BF16)
    rest = near - first.astype(F32)
    second = rest.astype(BF16)
    third = (rest - second.astype(F32)).astype(BF16)
    pieces = jnp.concatenate([first, second, third], axis=0)
    device_iota = lax.broadcasted_iota(jnp.int32, (device_count, lanes), 0)
    row_iota = lax.broadcasted_iota(jnp.int32, (rows, lanes), 0)
    lane = lax.broadcasted_iota(jnp.int32, (1, lanes), 1)
    query = lane & (queries - 1)
    device_lane = lax.broadcasted_iota(jnp.int32, (rows, device_count), 1)
    plane = busiest - (busiest & (PLANE - 1))
    sums = []
    for half in range(2):
        total = jnp.zeros((rows, 1), F32)
        for seat in range(half * PLANE // 2, (half + 1) * PLANE // 2):
            mine = jnp.sum(
                jnp.where(device_lane == plane + seat, far, 0.0), axis=1, keepdims=True
            )
            if seat:
                cut = rows - seat * part
                mine = jnp.concatenate([mine[cut:], mine[:cut]], axis=0)
            total = total + mine
        sums.append(total)
    values = []
    for s in range(per):
        holder = holder_ref[s : s + 1]
        mark = jnp.where(device_iota == holder, 1.0, 0.0).astype(BF16)
        three = jnp.dot(pieces, mark, preferred_element_type=F32)
        away = (three[:rows] + three[rows : 2 * rows]) + three[2 * rows :]
        hot = (holder == busiest) & ((query == first_hot) | (query == second_hot))
        extra = jnp.where(query == first_hot, sums[0], sums[1])
        found = jnp.where(hot, extra, away)
        row = jnp.where(hot, row_ref[s : s + 1], turned_ref[s : s + 1])
        value = jnp.sum(jnp.where(row_iota == row, found, 0.0), axis=0, keepdims=True)
        values.append(jnp.where(holder >= 0, value, 0.0))
    values = jnp.concatenate(values, axis=0)
    for g in range(slots // per):
        out_ref[g * per : (g + 1) * per, :] = values[:, g * queries : (g + 1) * queries]


def finish(note, holder, row, turned, back, slots, queries):
    return pl.pallas_call(
        finish_kernel,
        name="finish",
        out_shape=jax.ShapeDtypeStruct((slots, queries), F32),
        in_specs=[vmem(), vmem(), vmem(), vmem(), vmem()],
        out_specs=vmem(),
    )(near(note), near(holder), near(row), near(turned), near(back))


def turn(value, hop, planes):
    pairs = [
        (p * PLANE + s, p * PLANE + (s + hop) % PLANE)
        for p in range(planes) for s in range(PLANE)
    ]
    return lax.ppermute(value, "shard", pairs)


def local(
    query_tokens, candidates, cand_count, placement_map,
    passage_base, residual_codes, passage_lengths, bucket_weights,
):
    device_count = lax.axis_size("shard")
    planes = device_count // PLANE
    seat = lax.rem(lax.axis_index("shard"), PLANE).astype(jnp.int32).reshape(1)
    store_rows = passage_base.shape[0]
    store = decode(seat, passage_base, residual_codes, passage_lengths, bucket_weights)
    parts = [store[0]] + [turn(store[k], k, planes) for k in range(1, PLANE)]
    outgoing, holder, row, turned, note, busiest = prepare(
        candidates, cand_count, placement_map, query_tokens, store_rows, device_count
    )
    arrived = lax.all_to_all(outgoing, "shard", 0, 0, tiled=True)
    wanted = lax.rem(seat[0] - lax.rem(busiest[0], PLANE) + PLANE, PLANE)
    piece = parts[0]
    for k in range(1, PLANE):
        piece = jnp.where(wanted == k, parts[k], piece)
    hot_parts = [piece] + [turn(piece, -k, planes) for k in range(1, PLANE)]
    visited = score(arrived, store, hot_parts)
    back = lax.all_to_all(visited, "shard", 0, 0, tiled=True)
    queries, slots = candidates.shape
    return jnp.transpose(finish(note, holder, row, turned, back, slots, queries))


def solution(mesh):
    whole = P(("groups", "shard"))
    return jax.shard_map(
        local,
        mesh=mesh,
        in_specs=(whole, whole, whole, P("groups"), whole, whole, whole, P("groups")),
        out_specs=whole,
        check_vma=False,
    )
```

```python
import functools

import jax
import jax.numpy as jnp
from jax import lax
from jax.experimental import pallas as pl
from jax.experimental.pallas import tpu as pltpu
from jax.sharding import PartitionSpec as P

EPSILON = 1e-06
PLANE = 8
F32 = jnp.float32
BF16 = jnp.bfloat16


def vmem(*_):
    return pl.BlockSpec(memory_space=pltpu.VMEM)


def near(value):
    return pltpu.with_memory_space_constraint(value, pltpu.VMEM)


def smem(*_):
    return pl.BlockSpec(memory_space=pltpu.SMEM)


def cost(flops, moved):
    return pl.CostEstimate(flops=flops, transcendentals=0, bytes_accessed=moved)


def log2(value):
    assert value & (value - 1) == 0
    return value.bit_length() - 1


def prepare_kernel(
    store_rows, device_count,
    cand_ref, count_ref, map_ref, query_ref,
    out_ref, holder_ref, row_ref, turned_ref, note_ref, busiest_ref,
    present_ref, pick_vmem, pick_smem, sem, tokens_ref, packed_ref, in_sem, out_sem,
):
    load = pltpu.make_async_copy(query_ref, tokens_ref, in_sem)
    load.start()
    slots, queries = cand_ref.shape
    table_rows, lanes = map_ref.shape
    groups = lanes // queries
    per = slots // groups
    part_bits = log2(store_rows // PLANE)
    table = map_ref[...]
    holder_table = lax.shift_right_logical(table, log2(store_rows))
    row_table = table & (store_rows - 1)
    both = jnp.concatenate([holder_table, row_table], axis=1).astype(F32)
    both = jnp.transpose(both).astype(BF16)
    ids = cand_ref[...]
    ids = jnp.concatenate([ids[g * per : (g + 1) * per] for g in range(groups)], axis=1)
    count = jnp.concatenate([count_ref[...]] * groups, axis=1)
    high = lax.shift_right_logical(ids, log2(lanes))
    low = ids & (lanes - 1)
    lane = lax.broadcasted_iota(jnp.int32, (1, lanes), 1)
    first_slot = lax.shift_right_logical(lane, log2(queries)) * per
    table_iota = lax.broadcasted_iota(jnp.int32, (table_rows, lanes), 0)
    low_iota = lax.broadcasted_iota(jnp.int32, (lanes, lanes), 0)
    device_iota = lax.broadcasted_iota(jnp.int32, (device_count, lanes), 0)
    present = jnp.zeros((device_count, lanes), F32)
    for s in range(per):
        mark = jnp.where(table_iota == high[s : s + 1], 1.0, 0.0).astype(BF16)
        got = jnp.dot(both, mark, preferred_element_type=F32)
        here = low_iota == low[s : s + 1]
        holder = jnp.sum(jnp.where(here, got[:lanes], 0.0), axis=0, keepdims=True)
        row = jnp.sum(jnp.where(here, got[lanes:], 0.0), axis=0, keepdims=True)
        row = row.astype(jnp.int32)
        holder = jnp.where(first_slot + s < count, holder.astype(jnp.int32), -1)
        present = jnp.where(device_iota == holder, 1.0, present)
        block = (lax.shift_right_logical(row, part_bits) - holder) & (PLANE - 1)
        holder_ref[s : s + 1] = holder
        row_ref[s : s + 1] = row
        turned_ref[s : s + 1] = (block << part_bits) + (row & ((1 << part_bits) - 1))
    shift = queries
    while shift < lanes:
        present = jnp.maximum(present, pltpu.roll(present, shift, 1))
        shift *= 2
    present = jnp.where(lane < queries, present, 0.0)
    present_ref[...] = present
    kind = lax.broadcasted_iota(jnp.int32, (16, lanes), 0)
    lane_all = lax.broadcasted_iota(jnp.int32, (16, lanes), 1)
    weigh = jnp.where(kind == 0, lane_all, jnp.where(kind == 1, 1, 0))
    sums = lax.dot_general(
        weigh.astype(F32).astype(BF16), present.astype(BF16),
        (((1,), (1,)), ((), ())), preferred_element_type=F32,
    )
    pick_vmem[...] = jnp.clip(sums[0:1].astype(jnp.int32), 0, queries - 1)
    copy = pltpu.make_async_copy(pick_vmem, pick_smem, sem)
    copy.start()
    device = lax.broadcasted_iota(jnp.int32, (1, device_count), 1)
    busiest = jnp.max(jnp.where(sums[1:2] > 1.5, device.astype(F32), 0.0)).astype(jnp.int32)
    theirs = present_ref[pl.ds(busiest, 1), :]
    lane_f = lane.astype(F32)
    last = jnp.max(theirs * lane_f).astype(jnp.int32)
    first = queries - 1 - jnp.max(theirs * (queries - 1 - lane_f)).astype(jnp.int32)
    middle = jnp.sum(theirs * lane_f).astype(jnp.int32) - first - last
    middle = jnp.clip(middle, 0, queries - 1)
    busiest_ref[0] = busiest
    kind = lax.broadcasted_iota(jnp.int32, (8, device_count), 0)
    note_ref[...] = jnp.where(kind == 0, busiest, jnp.where(kind == 1, first, middle))
    tokens = query_ref.shape[1]
    extra = 2 * tokens // PLANE
    load.wait()
    spare = []
    for seat in range(PLANE):
        query = first if seat < PLANE // 2 else middle
        start = (seat % (PLANE // 2)) * extra
        spare.append(tokens_ref[query, start : start + extra, :])

    def pack_extra(step, carry):
        for seat in range(PLANE):
            packed_ref[step * PLANE + seat, tokens : tokens + extra, :] = spare[seat]
        return carry

    lax.fori_loop(0, device_count // PLANE, pack_extra, 0)
    copy.wait()
    pick_smem[0, busiest] = jnp.clip(last, 0, queries - 1)
    chunks = 8
    size = device_count // chunks
    stores = []
    for chunk in range(chunks):

        def pack(step, carry):
            for seat in range(PLANE):
                device = chunk * size + step * PLANE + seat
                packed_ref[device, 0:tokens, :] = tokens_ref[pick_smem[0, device]]
            return carry

        lax.fori_loop(0, size // PLANE, pack, 0)
        here = pl.ds(chunk * size, size)
        store = pltpu.make_async_copy(packed_ref.at[here], out_ref.at[here], out_sem.at[chunk])
        store.start()
        stores.append(store)
    for store in stores:
        store.wait()


def prepare(candidates, cand_count, placement_map, query_tokens, store_rows, device_count):
    queries, slots = candidates.shape
    _, tokens, dim = query_tokens.shape
    wide = pltpu.VMEM((slots * queries // dim, dim), jnp.int32)
    return pl.pallas_call(
        functools.partial(prepare_kernel, store_rows, device_count),
        name="prepare",
        out_shape=(
            jax.ShapeDtypeStruct((device_count, tokens + 2 * tokens // PLANE, dim), BF16),
            wide, wide, wide,
            pltpu.VMEM((8, device_count), jnp.int32),
            jax.ShapeDtypeStruct((1,), jnp.int32),
        ),
        in_specs=[vmem(), vmem(), vmem(), pl.BlockSpec(memory_space=pl.ANY)],
        out_specs=(pl.BlockSpec(memory_space=pl.ANY), vmem(), vmem(), vmem(), vmem(), smem()),
        scratch_shapes=[
            pltpu.VMEM((device_count, dim), F32),
            pltpu.VMEM((1, device_count), jnp.int32),
            pltpu.SMEM((1, device_count), jnp.int32),
            pltpu.SemaphoreType.DMA(()),
            pltpu.VMEM((queries, tokens, dim), BF16),
            pltpu.VMEM((device_count, tokens + 2 * tokens // PLANE, dim), BF16),
            pltpu.SemaphoreType.DMA(()),
            pltpu.SemaphoreType.DMA((8,)),
        ],
        cost_estimate=cost(10**9, 2 * 10**6),
    )(
        jnp.transpose(candidates),
        cand_count.reshape(1, queries),
        placement_map.reshape(-1, dim),
        query_tokens,
    )


def decode_kernel(seat_ref, length_ref, level_ref, base_ref, code_ref, out_ref):
    part, length, dim = base_ref.shape
    block = lax.rem(seat_ref[0] + pl.program_id(0), PLANE)
    token = lax.broadcasted_iota(jnp.int32, (length, dim), 0)
    for index in range(part):
        code = code_ref[index]
        residual = jnp.where(
            code < 2,
            jnp.where(code == 0, level_ref[0], level_ref[1]),
            jnp.where(code == 2, level_ref[2], level_ref[3]),
        )
        summed = base_ref[index].astype(F32) + residual
        inverse = lax.rsqrt(jnp.sum(summed * summed, axis=1, keepdims=True) + EPSILON)
        tokens = summed * inverse
        tokens = jnp.where(token < length_ref[block * part + index], tokens, tokens[0:1])
        out_ref[0, index] = tokens.astype(BF16)


def decode(seat, passage_base, residual_codes, passage_lengths, bucket_weights):
    rows, length, dim = passage_base.shape
    part = rows // PLANE
    spec = pl.BlockSpec(
        (part, length, dim), lambda i, seat_ref: (lax.rem(seat_ref[0] + i, PLANE), 0, 0)
    )
    return pl.pallas_call(
        decode_kernel,
        name="decode",
        out_shape=jax.ShapeDtypeStruct((PLANE, part, length, dim), BF16),
        grid_spec=pltpu.PrefetchScalarGridSpec(
            num_scalar_prefetch=1,
            grid=(PLANE,),
            in_specs=[smem(), smem(), spec, spec],
            out_specs=pl.BlockSpec((1, part, length, dim), lambda i, _: (i, 0, 0, 0)),
        ),
        cost_estimate=cost(rows * length * dim * 20, rows * length * dim * 8),
    )(seat, passage_lengths, bucket_weights, passage_base, residual_codes)


def score_kernel(arrived_ref, store_ref, *refs):
    hot_refs, (out_ref, best_ref) = refs[:PLANE], refs[PLANE:]
    count, height, dim = arrived_ref.shape
    _, part, length, _ = store_ref.shape
    rows = PLANE * part
    tokens = height * PLANE // (PLANE + 2)
    extra = height - tokens
    group = 256 // tokens
    slots = 256 // extra
    wide = 256

    def against(index, query, block):
        best = []
        for row in range(rows):
            similar = lax.dot_general(
                block(row // part, row % part), query, (((1,), (1,)), ((), ())),
                preferred_element_type=F32,
            )
            best.append(jnp.max(similar, axis=0, keepdims=True))
        best_ref[index] = jnp.concatenate(best, axis=0)

    blocks = count // slots
    inner_blocks = slots // group

    def some(step, carry):
        start = pl.multiple_of(step * slots, slots)
        for inner in range(inner_blocks):
            here = pl.ds(start + inner * group, group)
            query = arrived_ref[here, 0:tokens, :].reshape(wide, dim)
            against(step * inner_blocks + inner, query, lambda k, j: store_ref[k, j])
        query = arrived_ref[pl.ds(start, slots), tokens:height, :].reshape(wide, dim)
        against(blocks * inner_blocks + step, query, lambda k, j: hot_refs[k][j])
        return carry

    lax.fori_loop(0, blocks, some, 0)
    slot = lax.broadcasted_iota(jnp.int32, (wide, count), 1)
    token = lax.broadcasted_iota(jnp.int32, (wide, count), 0)

    def sums(first_block, number, span):
        member = lax.shift_right_logical(token, log2(span))
        total = jnp.zeros((3 * rows, count), F32)
        for index in range(number):
            best = best_ref[first_block + index]
            first = best.astype(BF16)
            rest = best - first.astype(F32)
            second = rest.astype(BF16)
            third = (rest - second.astype(F32)).astype(BF16)
            picks = jnp.where(slot == member + index * (wide // span), 1.0, 0.0).astype(BF16)
            total = total + jnp.dot(
                jnp.concatenate([first, second, third], axis=0), picks,
                preferred_element_type=F32,
            )
        return (total[:rows] + total[rows : 2 * rows]) + total[2 * rows :]

    near_sums = sums(0, blocks * inner_blocks, tokens)
    far_sums = sums(blocks * inner_blocks, blocks, extra)
    out_ref[...] = jnp.transpose(jnp.concatenate([near_sums, far_sums], axis=0))


def score(arrived, store, hot_parts):
    count, height, dim = arrived.shape
    _, part, length, _ = store.shape
    rows = PLANE * part
    return pl.pallas_call(
        score_kernel,
        name="score",
        compiler_params=pltpu.CompilerParams(vmem_limit_bytes=16 * 2**20),
        out_shape=pltpu.VMEM((count, 2 * rows), F32),
        in_specs=[vmem()] * (2 + PLANE),
        out_specs=vmem(),
        scratch_shapes=[pltpu.VMEM((count * height // 256, rows, 256), F32)],
        cost_estimate=cost(
            2 * count * height * rows * length * dim,
            2 * (count * height + 2 * rows * length) * dim,
        ),
    )(near(arrived), store, *[near(part) for part in hot_parts])


def finish_kernel(note_ref, holder_ref, row_ref, turned_ref, back_ref, out_ref):
    slots, queries = out_ref.shape
    per, lanes = holder_ref.shape
    device_count, double = back_ref.shape
    rows = double // 2
    part = rows // PLANE
    busiest = note_ref[0:1]
    first_hot = note_ref[1:2]
    second_hot = note_ref[2:3]
    back = jnp.transpose(back_ref[...])
    near, far = back[:rows], back[rows:]
    first = near.astype(BF16)
    rest = near - first.astype(F32)
    second = rest.astype(BF16)
    third = (rest - second.astype(F32)).astype(BF16)
    pieces = jnp.concatenate([first, second, third], axis=0)
    device_iota = lax.broadcasted_iota(jnp.int32, (device_count, lanes), 0)
    row_iota = lax.broadcasted_iota(jnp.int32, (rows, lanes), 0)
    lane = lax.broadcasted_iota(jnp.int32, (1, lanes), 1)
    query = lane & (queries - 1)
    device_lane = lax.broadcasted_iota(jnp.int32, (rows, device_count), 1)
    plane = busiest - (busiest & (PLANE - 1))
    sums = []
    for half in range(2):
        total = jnp.zeros((rows, 1), F32)
        for seat in range(half * PLANE // 2, (half + 1) * PLANE // 2):
            mine = jnp.sum(
                jnp.where(device_lane == plane + seat, far, 0.0), axis=1, keepdims=True
            )
            if seat:
                cut = rows - seat * part
                mine = jnp.concatenate([mine[cut:], mine[:cut]], axis=0)
            total = total + mine
        sums.append(total)
    values = []
    for s in range(per):
        holder = holder_ref[s : s + 1]
        mark = jnp.where(device_iota == holder, 1.0, 0.0).astype(BF16)
        three = jnp.dot(pieces, mark, preferred_element_type=F32)
        away = (three[:rows] + three[rows : 2 * rows]) + three[2 * rows :]
        hot = (holder == busiest) & ((query == first_hot) | (query == second_hot))
        extra = jnp.where(query == first_hot, sums[0], sums[1])
        found = jnp.where(hot, extra, away)
        row = jnp.where(hot, row_ref[s : s + 1], turned_ref[s : s + 1])
        value = jnp.sum(jnp.where(row_iota == row, found, 0.0), axis=0, keepdims=True)
        values.append(jnp.where(holder >= 0, value, 0.0))
    values = jnp.concatenate(values, axis=0)
    for g in range(slots // per):
        out_ref[g * per : (g + 1) * per, :] = values[:, g * queries : (g + 1) * queries]


def finish(note, holder, row, turned, back, slots, queries):
    return pl.pallas_call(
        finish_kernel,
        name="finish",
        out_shape=jax.ShapeDtypeStruct((slots, queries), F32),
        in_specs=[vmem(), vmem(), vmem(), vmem(), vmem()],
        out_specs=vmem(),
    )(near(note), near(holder), near(row), near(turned), near(back))


def turn(value, hop, planes):
    pairs = [
        (p * PLANE + s, p * PLANE + (s + hop) % PLANE)
        for p in range(planes) for s in range(PLANE)
    ]
    return lax.ppermute(value, "shard", pairs)


def local(
    query_tokens, candidates, cand_count, placement_map,
    passage_base, residual_codes, passage_lengths, bucket_weights,
):
    device_count = lax.axis_size("shard")
    planes = device_count // PLANE
    seat = lax.rem(lax.axis_index("shard"), PLANE).astype(jnp.int32).reshape(1)
    store_rows = passage_base.shape[0]
    store = decode(seat, passage_base, residual_codes, passage_lengths, bucket_weights)
    parts = [store[0]] + [turn(store[k], k, planes) for k in range(1, PLANE)]
    outgoing, holder, row, turned, note, busiest = prepare(
        candidates, cand_count, placement_map, query_tokens, store_rows, device_count
    )
    arrived = lax.all_to_all(outgoing, "shard", 0, 0, tiled=True)
    wanted = lax.rem(seat[0] - lax.rem(busiest[0], PLANE) + PLANE, PLANE)
    piece = parts[0]
    for k in range(1, PLANE):
        piece = jnp.where(wanted == k, parts[k], piece)
    hot_parts = [piece] + [turn(piece, -k, planes) for k in range(1, PLANE)]
    visited = score(arrived, store, hot_parts)
    back = lax.all_to_all(visited, "shard", 0, 0, tiled=True)
    queries, slots = candidates.shape
    return jnp.transpose(finish(note, holder, row, turned, back, slots, queries))


def solution(mesh):
    whole = P(("groups", "shard"))
    return jax.shard_map(
        local,
        mesh=mesh,
        in_specs=(whole, whole, whole, P("groups"), whole, whole, whole, P("groups")),
        out_specs=whole,
        check_vma=False,
    )
```
